256 devices in a mesh: dp: 16 (over z, x_lo), tp: 16 (over y, x_hi, core).
Axes of the slice: x: 4 (x_hi: 2, x_lo: 2; x = x_hi * 2 + x_lo), y: 4, z: 8, core: 2. Of those that a mesh axis runs over, the one named last changes fastest.
Arguments:
- queries: bfloat16 [8192, 8192], P('dp', 'tp'), parts along dimension 0, may hold values from -200 to 200
- new_keys: bfloat16 [8192, 1024], P('dp', 'tp'), parts along dimension 0, may hold values from -9 to 9
- new_values: bfloat16 [8192, 1024], P('dp', 'tp'), parts along dimension 0, may hold values from -60 to 60
- cache_keys: bfloat16 [64, 32768, 128], P('dp', 'tp'), parts along dimension 0, may hold values from -4 to 4
- cache_values: bfloat16 [64, 32768, 128], P('dp', 'tp'), parts along dimension 0, may hold values from -60 to 60
- out_weight: bfloat16 [8192, 8192], P('tp'), may hold values from -0.09375 to 0.09375
- residual: bfloat16 [8192, 8192], P('dp', 'tp'), parts along dimension 0, may hold values from -8 to 8
- norm_gain: bfloat16 [8192], P('tp'), may hold values from 0.5 to 1.5
Outputs:
- normed: bfloat16 [8192, 8192], P('dp', 'tp'), parts along dimension 0
The draws below stay inside these ranges and needn't reach their ends.
There are 16 independent parts, one for each index of `dp`. The reference program is written for one: setup_inputs(seed, part) draws one part's arguments, and reference() takes and returns one part's arrays. A program takes and returns all parts, laid end to end along the dimension named above; an argument that names none is the same for every part. Nothing has to cross between parts.
All inputs are finite; a program needn't handle non-finite values.
Results may differ from the reference program's by a relative error of at most 0.015.
Values may be sent and summed in bfloat16 or wider, within the bound.
A program may use at most 128 MiB of HBM per device.

```python
import math
import jax
import jax.numpy as jnp
from jax import lax

D = 8192
H = 64
KVH = 8
HD = 128
SPAN = 128
SEQS = 4
CTX = 4096
TOK = 512


def build_drawn(key):
    key_stored = jax.random.fold_in(key, 11)
    key_query = jax.random.fold_in(key, 12)
    stored = jax.random.truncated_normal(key_stored, -4.0, 4.0, (SEQS, KVH * CTX, HD), jnp.float32)
    asked = jax.random.truncated_normal(key_query, -4.0, 4.0, (SEQS * SPAN, H * HD), jnp.float32)
    return (stored, asked)


def draw_cache_keys(key, part):
    return build_drawn(key)[0].astype(jnp.bfloat16)


def draw_queries(key, part):
    return build_drawn(key)[1].astype(jnp.bfloat16)


def draw_residual(key, part):
    key_base = jax.random.fold_in(key, 21)
    position = jnp.arange(D, dtype=jnp.float32) / D
    rising = 0.15 * jnp.exp(position * math.log(3.0))
    values = jax.random.truncated_normal(key_base, -4.0, 4.0, (SEQS * SPAN, D), jnp.float32) * rising[None, :]
    return values.astype(jnp.bfloat16)


def spiked(values, own_key, source, target, parts, factor):
    owner, partner = [(jnp.arange(values.shape[dim]) // (values.shape[dim] // parts)).reshape([-1 if axis == dim else 1 for axis in range(values.ndim)]) for dim in (source, target)]
    chosen = jax.random.permutation(own_key, parts)[partner]
    strong = (owner == chosen) | (owner == (partner + parts // 2) % parts)
    return jnp.where(strong, factor * values, values)


def levels(own_key, shape, shards, low, high):
    factor_of = 1.0
    for dim, parts in shards:
        draws = jax.random.uniform(jax.random.fold_in(jax.random.fold_in(own_key, 6), dim), (parts,), jnp.float32, low / len(shards), high / len(shards))
        factor_of = factor_of * jnp.repeat(jnp.exp(draws), shape[dim] // parts).reshape((-1,) + (1,) * (len(shape) - 1 - dim))
    return factor_of


def scatter_about(own_key, shape, deviation, limit, split=(), held_as=jnp.bfloat16):
    drawn = jax.random.normal(own_key, shape, jnp.float32) * deviation
    if len(split) > 0:
        drawn = levels(own_key, shape, split, -0.22, 0.18) * drawn
    return jnp.clip(drawn, min=-limit, max=limit).astype(held_as)


def heavy_noise(stream_key, extent, spread, most, pieces, heavy, held_as=jnp.bfloat16):
    values = spread * jax.random.normal(stream_key, extent, jnp.float32)
    if pieces:
        values = values * levels(stream_key, extent, pieces, -0.22, 0.18)
    return jnp.clip(spiked(values, jax.random.fold_in(stream_key, 3), *heavy), -most, most).astype(held_as)


def setup_inputs(seed: int = 0, part: int = 0) -> dict:
    keys = jax.random.split(jax.random.key(seed), 9)
    part_splits = jax.random.split(jax.random.fold_in(keys[8], part), 9)
    queries = draw_queries(jax.random.fold_in(jax.random.fold_in(keys[8], part), 71), part)
    new_keys = scatter_about(part_splits[1], (TOK, KVH * HD), 1.5, 9.0, ((1, 16),))
    new_values = scatter_about(part_splits[2], (TOK, KVH * HD), 10.0, 60.0, ((1, 16),))
    cache_keys = draw_cache_keys(jax.random.fold_in(jax.random.fold_in(keys[8], part), 71), part)
    cache_values = scatter_about(part_splits[4], (SEQS, KVH * CTX, HD), 10.0, 60.0, ((1, 16),))
    out_weight = heavy_noise(keys[5], (H * HD, D), (H * HD) ** -0.5, 0.09375, ((0, 16),), (0, 1, 16, 2.0))
    residual = draw_residual(jax.random.fold_in(jax.random.fold_in(keys[8], part), 71), part)
    norm_gain = jnp.clip(1.0 + 0.1 * jax.random.normal(keys[7], (D,), jnp.float32), 0.5, 1.5).astype(jnp.bfloat16)
    return {"queries": queries, "new_keys": new_keys, "new_values": new_values, "cache_keys": cache_keys, "cache_values": cache_values, "out_weight": out_weight, "residual": residual, "norm_gain": norm_gain}


def attend_sequence(inputs):
    query_rows, fresh_keys, fresh_values, stored_keys, stored_values = inputs
    groups = H // KVH
    scaling = HD ** (-0.5)
    grouped = query_rows.astype(jnp.float32).reshape(SPAN, KVH, groups, HD)
    old_keys = stored_keys.astype(jnp.float32).reshape(KVH, CTX, HD)
    old_values = stored_values.astype(jnp.float32).reshape(KVH, CTX, HD)
    recent_keys = fresh_keys.astype(jnp.float32).reshape(SPAN, KVH, HD)
    recent_values = fresh_values.astype(jnp.float32).reshape(SPAN, KVH, HD)
    old_scores = jnp.einsum('ighd,gjd->ghij', grouped, old_keys) * scaling
    recent_scores = jnp.einsum('ighd,jgd->ghij', grouped, recent_keys) * scaling
    causal = jnp.arange(SPAN)[:, None] >= jnp.arange(SPAN)[None, :]
    recent_scores = jnp.where(causal, recent_scores, -jnp.inf)
    peak = jnp.maximum(lax.optimization_barrier(jnp.max(old_scores, axis=-1)), lax.optimization_barrier(jnp.max(recent_scores, axis=-1)))
    old_weights = jnp.exp(old_scores - peak[..., None])
    recent_weights = jnp.exp(recent_scores - peak[..., None])
    total = lax.optimization_barrier(jnp.sum(old_weights, axis=-1)) + lax.optimization_barrier(jnp.sum(recent_weights, axis=-1))
    rounded_old = lax.optimization_barrier(old_weights.astype(jnp.bfloat16)).astype(jnp.float32)
    rounded_recent = lax.optimization_barrier(recent_weights.astype(jnp.bfloat16)).astype(jnp.float32)
    mixed = jnp.einsum('ghij,gjd->ighd', rounded_old, old_values)
    mixed = mixed + jnp.einsum('ghij,jgd->ighd', rounded_recent, recent_values)
    result = mixed / jnp.transpose(total, (2, 0, 1))[..., None]
    return result.reshape(SPAN, H * HD).astype(jnp.bfloat16)

def reference(queries, new_keys, new_values, cache_keys, cache_values, out_weight, residual, norm_gain):
    inputs = (queries.reshape(SEQS, SPAN, H * HD), new_keys.reshape(SEQS, SPAN, KVH * HD), new_values.reshape(SEQS, SPAN, KVH * HD), cache_keys, cache_values)
    attended = lax.map(attend_sequence, inputs).reshape(SEQS * SPAN, H * HD)
    projected = jnp.dot(attended, out_weight, preferred_element_type=jnp.float32)
    hidden = residual.astype(jnp.float32) + projected
    power = lax.optimization_barrier(jnp.mean(hidden * hidden, axis=1, keepdims=True))
    normed = hidden * lax.rsqrt(power + 1e-05) * norm_gain.astype(jnp.float32)
    return normed.astype(jnp.bfloat16)
```

```python
import jax
import jax.numpy as jnp
from jax import lax
from jax.experimental import pallas as pl
from jax.experimental.pallas import tpu as pltpu
from jax.sharding import PartitionSpec as P

D = 8192
HD = 128
SPAN = 128
SEQS = 4
HALF = 2048
COLS = 512
EPSILON = 1e-05
SCALE = HD**-0.5 * 1.4426950408889634

MESH = pl.DeviceIdType.MESH
F32 = jnp.float32
BF16 = jnp.bfloat16

ORDER = ((2, 0), (2, 1), (1, 1), (3, 0), (1, 0), (3, 1), (0, 1), (0, 0))


def dot_t(a, b):
    return lax.dot_general(a, b, (((1,), (1,)), ((), ())), preferred_element_type=F32)


def dot(a, b):
    return jnp.dot(a, b, preferred_element_type=F32)


def with_ones(v):
    return jnp.concatenate([v, jnp.ones_like(v)], axis=1)


def kernel(
    q_hbm, nk_hbm, nv_hbm, ck_hbm, cv_hbm, w_hbm, res_hbm, gain_ref, out_ref,
    q_v, kown, vown, koth, voth, nk_own, nv_own, nk_oth, nv_oth, nk, nv,
    wown, woth, m_ref, acc_ref, aown, aoth, pbuf, fbuf, xbuf, r1, r2, rx,
    hid, res_v, ss, ssr,
    load_sem, kvl_sem, wl_sem,
    kv_send, kv_recv, nkv_send, nkv_recv, w_send, w_recv, a_send, a_recv,
    r1_send, r1_recv, r2_send, r2_recv, x_send, x_recv, ss_send, ss_recv,
):
    me = lax.axis_index("tp")
    core = lax.rem(me, 2)
    xh = lax.rem(lax.div(me, 2), 2)
    y = lax.div(me, 4)

    def peer(dy, dx, dc):
        py = lax.rem(y + dy, 4)
        px = lax.rem(xh + dx, 2)
        pc = lax.rem(core + dc, 2)
        return (py * 2 + px) * 2 + pc

    partner = peer(0, 0, 1)
    up, down, far, across = peer(1, 0, 0), peer(3, 0, 0), peer(2, 0, 0), peer(0, 1, 0)

    def remote(src, dst, send, recv, dev):
        return pltpu.make_async_remote_copy(
            src_ref=src, dst_ref=dst, send_sem=send, recv_sem=recv,
            device_id={"tp": dev}, device_id_type=MESH,
        )

    def kv_local(s):
        return (
            pltpu.make_async_copy(ck_hbm.at[s], kown.at[s], kvl_sem.at[s, 0]),
            pltpu.make_async_copy(cv_hbm.at[s], vown.at[s], kvl_sem.at[s, 1]),
        )

    def kv_remote(s):
        return (
            remote(ck_hbm.at[s], koth.at[s], kv_send.at[s, 0], kv_recv.at[s, 0], partner),
            remote(cv_hbm.at[s], voth.at[s], kv_send.at[s, 1], kv_recv.at[s, 1], partner),
        )

    def columns(slot, dc):
        dy, dx = ORDER[slot]
        start = peer(dy, dx, dc) * COLS
        return w_hbm.at[:, pl.ds(pl.multiple_of(start, COLS), COLS)]

    def w_local(slot):
        return pltpu.make_async_copy(columns(slot, 0), wown.at[slot], wl_sem.at[slot])

    def w_remote(slot):
        return remote(
            columns(slot, 1), woth.at[slot], w_send.at[slot], w_recv.at[slot], partner
        )

    def nkv_remote():
        return (
            remote(nk_hbm, nk_oth, nkv_send.at[0], nkv_recv.at[0], partner),
            remote(nv_hbm, nv_oth, nkv_send.at[1], nkv_recv.at[1], partner),
        )

    def attended_remote(s):
        return remote(aown.at[s], aoth.at[s], a_send.at[s], a_recv.at[s], partner)

    def first_remote(s):
        return (
            remote(pbuf.at[s, 0], r1.at[s, 0], r1_send.at[s, 0], r1_recv.at[s, 0], up),
            remote(pbuf.at[s, 1], r1.at[s, 1], r1_send.at[s, 1], r1_recv.at[s, 1], down),
        )

    def direct_remote(s):
        return (
            remote(pbuf.at[s, 2], r2.at[s, 1], r2_send.at[s, 1], r2_recv.at[s, 1], up),
            remote(pbuf.at[s, 3], r2.at[s, 2], r2_send.at[s, 2], r2_recv.at[s, 2], down),
        )

    def forward_remote(s):
        return (
            remote(fbuf.at[s, 0], r2.at[s, 0], r2_send.at[s, 0], r2_recv.at[s, 0], up),
            remote(fbuf.at[s, 1], r2.at[s, 3], r2_send.at[s, 3], r2_recv.at[s, 3], down),
        )

    def x_remote(s):
        return remote(xbuf.at[s], rx.at[s], x_send.at[s], x_recv.at[s], across)

    load = (
        pltpu.make_async_copy(q_hbm, q_v, load_sem.at[0]),
        pltpu.make_async_copy(nk_hbm, nk_own, load_sem.at[1]),
        pltpu.make_async_copy(nv_hbm, nv_own, load_sem.at[2]),
        pltpu.make_async_copy(res_hbm, res_v, load_sem.at[3]),
    )

    barrier = pltpu.get_barrier_semaphore()
    for dev in (partner, up, down, far, across):
        pl.semaphore_signal(barrier, inc=1, device_id={"tp": dev}, device_id_type=MESH)
    load[0].start()
    for copy in kv_local(0):
        copy.start()
    load[1].start()
    load[2].start()
    pl.semaphore_wait(barrier, 5)

    for copy in kv_remote(0) + nkv_remote():
        copy.start()
    for slot in range(4):
        w_remote(slot).start()
    for s in range(1, SEQS):
        for copy in kv_local(s):
            copy.start()
    for slot in range(8):
        w_local(slot).start()
    load[3].start()

    def rows_of(s):
        part = q_v[pl.ds(pl.multiple_of(s * SPAN, SPAN), SPAN), :]
        return jnp.concatenate([part[:, h * HD : (h + 1) * HD] for h in range(4)], axis=0)

    def own_half(s):
        for copy in kv_local(s):
            copy.wait()
        scores = dot_t(rows_of(s), kown[s])
        peak = jnp.max(scores, axis=1, keepdims=True)
        weights = jnp.exp2((scores - peak) * SCALE).astype(BF16)
        acc_ref[...] = dot(weights, with_ones(vown[s]))
        m_ref[...] = jnp.broadcast_to(peak, m_ref.shape)

    def other_half(s):
        for copy in kv_remote(s):
            copy.wait_recv()
        q = rows_of(s)
        tokens = pl.ds(pl.multiple_of(s * SPAN, SPAN), SPAN)
        scores = dot_t(q, koth[s])
        recent = dot_t(q, nk[tokens, :])
        row = lax.rem(lax.broadcasted_iota(jnp.int32, recent.shape, 0), SPAN)
        col = lax.broadcasted_iota(jnp.int32, recent.shape, 1)
        recent = jnp.where(row >= col, recent, -jnp.inf)
        old = m_ref[:, :1]
        peak = jnp.maximum(
            jnp.max(scores, axis=1, keepdims=True), jnp.max(recent, axis=1, keepdims=True)
        )
        peak = jnp.maximum(peak, old)
        weights = jnp.exp2((scores - peak) * SCALE).astype(BF16)
        recent_weights = jnp.exp2((recent - peak) * SCALE).astype(BF16)
        mixed = acc_ref[...] * jnp.exp2((old - peak) * SCALE)
        mixed = mixed + dot(weights, with_ones(voth[s]))
        mixed = mixed + dot(recent_weights, with_ones(nv[tokens, :]))
        result = (mixed[:, :HD] / mixed[:, HD:]).astype(BF16)
        for h in range(4):
            aown[s, :, h * HD : (h + 1) * HD] = result[h * SPAN : (h + 1) * SPAN, :]

    def project(s):
        attended_remote(s).wait_recv()
        for slot in range(8):
            block = dot(aown[s], wown[slot]) + dot(aoth[s], woth[slot])
            pbuf[s, slot] = block.astype(BF16)
            if slot < 2:
                first_remote(s)[slot].start()
            elif slot < 4:
                direct_remote(s)[slot - 2].start()

    def forward(s):
        for i, copy in enumerate(first_remote(s)):
            copy.wait_recv()
            fbuf[s, i] = (r1[s, i].astype(F32) + pbuf[s, 4 + i].astype(F32)).astype(BF16)
            forward_remote(s)[i].start()

    def send_across(s):
        direct_remote(s)[0].wait_recv()
        forward_remote(s)[1].wait_recv()
        total = pbuf[s, 6].astype(F32) + r2[s, 1].astype(F32) + r2[s, 3].astype(F32)
        xbuf[s] = total.astype(BF16)
        x_remote(s).start()

    def to_row(column):
        return jnp.transpose(jnp.broadcast_to(column, (SPAN, SPAN)))[:8, :]

    def finish(s):
        direct_remote(s)[1].wait_recv()
        forward_remote(s)[0].wait_recv()
        x_remote(s).wait_recv()
        tokens = pl.ds(pl.multiple_of(s * SPAN, SPAN), SPAN)
        total = pbuf[s, 7].astype(F32) + r2[s, 0].astype(F32) + r2[s, 2].astype(F32)
        total = total + rx[s].astype(F32) + res_v[tokens, :].astype(F32)
        hid[s] = total
        ss[0, s] = to_row(jnp.sum(total * total, axis=1, keepdims=True))

    load[0].wait()
    own_half(0)

    for copy in load[1:3]:
        copy.wait()
    for copy in nkv_remote():
        copy.wait_recv()
    lane = lax.broadcasted_iota(jnp.int32, (64, HD), 1)
    line = lax.broadcasted_iota(jnp.int32, (64, HD), 0)
    mine = (lane == line + 64 * core).astype(F32).astype(BF16)
    theirs = (lane == line + 64 * (1 - core)).astype(F32).astype(BF16)
    nk[...] = (dot(nk_own[...], mine) + dot(nk_oth[...], theirs)).astype(BF16)
    nv[...] = (dot(nv_own[...], mine) + dot(nv_oth[...], theirs)).astype(BF16)
    for slot in range(8):
        w_local(slot).wait()
    load[3].wait()

    def sequence(s, carry):
        other_half(s)
        attended_remote(s).start()

        @pl.when(s == 0)
        def _():
            for slot in range(4, 8):
                w_remote(slot).start()

        @pl.when(s < SEQS - 1)
        def _():
            for copy in kv_remote(s + 1):
                copy.start()
            own_half(s + 1)

        @pl.when(s >= 1)
        def _():
            forward(s - 1)

        @pl.when(s >= 2)
        def _():
            send_across(s - 2)

        @pl.when(s == 0)
        def _():
            for slot in range(8):
                w_remote(slot).wait_recv()

        project(s)
        return carry

    lax.fori_loop(0, SEQS, sequence, 0)

    forward(SEQS - 1)
    send_across(SEQS - 2)
    finish(0)
    finish(1)
    send_across(SEQS - 1)
    finish(2)
    finish(3)

    def exchange(i, source, dev):
        return remote(ss.at[source], ssr.at[i], ss_send.at[i], ss_recv.at[i], dev)

    copies = [exchange(0, 0, partner)]
    copies[0].start()
    copies[0].wait_recv()
    ss[1] = ss[0] + ssr[0]
    copies.append(exchange(1, 1, across))
    copies[1].start()
    copies[1].wait_recv()
    ss[2] = ss[1] + ssr[1]
    for i, dev in enumerate((up, down, far)):
        copies.append(exchange(2 + i, 2, dev))
        copies[-1].start()
    for copy in copies[2:]:
        copy.wait_recv()
    ss[3] = ss[2] + ssr[2] + ssr[3] + ssr[4]

    for s in range(SEQS):
        row = lax.rsqrt(ss[3, s] * (1.0 / D) + EPSILON)[:1, :]
        column = jnp.transpose(jnp.broadcast_to(row, (SPAN, SPAN)))[:, :1]
        out_ref[s * SPAN : (s + 1) * SPAN, :] = (hid[s] * column * gain_ref[...]).astype(BF16)

    for copy in copies:
        copy.wait_send()
    for copy in nkv_remote():
        copy.wait_send()
    for slot in range(8):
        w_remote(slot).wait_send()

    def drain(s, carry):
        for copy in kv_remote(s) + first_remote(s) + direct_remote(s) + forward_remote(s):
            copy.wait_send()
        attended_remote(s).wait_send()
        x_remote(s).wait_send()
        return carry

    lax.fori_loop(0, SEQS, drain, 0)


def per_device(queries, new_keys, new_values, cache_keys, cache_values, out_weight, residual, gain):
    any_spec = pl.BlockSpec(memory_space=pl.ANY)
    vmem_spec = pl.BlockSpec(memory_space=pltpu.VMEM)
    dma = pltpu.SemaphoreType.DMA
    block = (SPAN, COLS)
    return pl.pallas_call(
        kernel,
        name="attend",
        out_shape=jax.ShapeDtypeStruct((SEQS * SPAN, COLS), BF16),
        in_specs=[any_spec] * 7 + [vmem_spec],
        out_specs=vmem_spec,
        scratch_shapes=[
            pltpu.VMEM((SEQS * SPAN, 4 * HD), BF16),
            *[pltpu.VMEM((SEQS, HALF, HD), BF16)] * 4,
            *[pltpu.VMEM((SEQS * SPAN, HD // 2), BF16)] * 4,
            *[pltpu.VMEM((SEQS * SPAN, HD), BF16)] * 2,
            *[pltpu.VMEM((8, COLS, COLS), BF16)] * 2,
            pltpu.VMEM((4 * SPAN, HD), F32),
            pltpu.VMEM((4 * SPAN, 2 * HD), F32),
            *[pltpu.VMEM((SEQS, *block), BF16)] * 2,
            pltpu.VMEM((SEQS, 8, *block), BF16),
            pltpu.VMEM((SEQS, 2, *block), BF16),
            pltpu.VMEM((SEQS, *block), BF16),
            pltpu.VMEM((SEQS, 2, *block), BF16),
            pltpu.VMEM((SEQS, 4, *block), BF16),
            pltpu.VMEM((SEQS, *block), BF16),
            pltpu.VMEM((SEQS, *block), F32),
            pltpu.VMEM((SEQS * SPAN, COLS), BF16),
            pltpu.VMEM((4, SEQS, 8, SPAN), F32),
            pltpu.VMEM((5, SEQS, 8, SPAN), F32),
            dma((4,)), dma((SEQS, 2)), dma((8,)),
            dma((SEQS, 2)), dma((SEQS, 2)), dma((2,)), dma((2,)),
            dma((8,)), dma((8,)), dma((SEQS,)), dma((SEQS,)),
            dma((SEQS, 2)), dma((SEQS, 2)), dma((SEQS, 4)), dma((SEQS, 4)),
            dma((SEQS,)), dma((SEQS,)), dma((5,)), dma((5,)),
        ],
        compiler_params=pltpu.CompilerParams(
            collective_id=0, has_side_effects=True, vmem_limit_bytes=60 * 2**20
        ),
    )(
        queries, new_keys, new_values, cache_keys, cache_values, out_weight, residual,
        gain.astype(F32)[None, :],
    )


def solution(mesh):
    in_specs = (
        P("dp", "tp"),
        P("dp", "tp"),
        P("dp", "tp"),
        P("dp", "tp", None),
        P("dp", "tp", None),
        P("tp", None),
        P("dp", "tp"),
        P("tp"),
    )
    return jax.shard_map(
        per_device, mesh=mesh, in_specs=in_specs, out_specs=P("dp", "tp"), check_vma=False
    )
```

```python
import jax
import jax.numpy as jnp
from jax import lax
from jax.experimental import pallas as pl
from jax.experimental.pallas import tpu as pltpu
from jax.sharding import PartitionSpec as P

D = 8192
HD = 128
SPAN = 128
SEQS = 4
HALF = 2048
COLS = 512
EPSILON = 1e-05
SCALE = HD**-0.5 * 1.4426950408889634

MESH = pl.DeviceIdType.MESH
F32 = jnp.float32
BF16 = jnp.bfloat16

ORDER = ((2, 1), (2, 0), (1, 1), (3, 0), (3, 1), (0, 1), (1, 0), (0, 0))
SLOT = {key: slot for slot, key in enumerate(ORDER)}
WIDE = COLS // 2
HEADS = 2
ROWS = HEADS * SPAN
CHUNKS = 4 // HEADS
TALL = SPAN // 2


def dot_t(a, b):
    return lax.dot_general(a, b, (((1,), (1,)), ((), ())), preferred_element_type=F32)


def dot(a, b):
    return jnp.dot(a, b, preferred_element_type=F32)


def with_ones(v, axis=1):
    return jnp.concatenate([v, jnp.ones_like(v)], axis=axis)


def kernel(
    q_hbm, nk_hbm, nv_hbm, ck_hbm, cv_hbm, w_hbm, res_hbm, gain_ref, out_ref,
    q_v, kown, vown, koth, voth, nk, nv, wown, woth, m_ref, acc_ref, aown, aoth,
    pbuf, fbuf, xbuf, r1, r2, rx, rxx, cbuf, gbuf, q1, q2, hid, res_v, ss, ssr,
    load_sem, kvl_sem, wl_sem,
    kv_send, kv_recv, nkv_send, nkv_recv, w_send, w_recv, a_send, a_recv,
    r1_send, r1_recv, r2_send, r2_recv, x_send, x_recv, xx_send, xx_recv,
    q1_send, q1_recv, q2_send, q2_recv, ss_send, ss_recv,
):
    me = lax.axis_index("tp")
    core = lax.rem(me, 2)
    xh = lax.rem(lax.div(me, 2), 2)
    y = lax.div(me, 4)
    half = pl.ds(pl.multiple_of(core * (HD // 2), HD // 2), HD // 2)

    def peer(dy, dx, dc):
        py = lax.rem(y + dy, 4)
        px = lax.rem(xh + dx, 2)
        pc = lax.rem(core + dc, 2)
        return (py * 2 + px) * 2 + pc

    partner = peer(0, 0, 1)
    up, down, far, across = peer(1, 0, 0), peer(3, 0, 0), peer(2, 0, 0), peer(0, 1, 0)

    def remote(src, dst, send, recv, dev):
        return pltpu.make_async_remote_copy(
            src_ref=src, dst_ref=dst, send_sem=send, recv_sem=recv,
            device_id={"tp": dev}, device_id_type=MESH,
        )

    def kv_local(s):
        return (
            pltpu.make_async_copy(ck_hbm.at[s], kown.at[s], kvl_sem.at[s, 0]),
            pltpu.make_async_copy(cv_hbm.at[s], vown.at[s], kvl_sem.at[s, 1]),
        )

    def kv_remote(s):
        return (
            remote(ck_hbm.at[s], koth.at[s], kv_send.at[s, 0], kv_recv.at[s, 0], partner),
            remote(cv_hbm.at[s], voth.at[s], kv_send.at[s, 1], kv_recv.at[s, 1], partner),
        )

    def columns(slot, dc):
        dy, dx = ORDER[slot]
        start = peer(dy, dx, dc) * COLS
        return w_hbm.at[:, pl.ds(pl.multiple_of(start, COLS), COLS)]

    def w_local(slot):
        return pltpu.make_async_copy(columns(slot, 0), wown.at[slot], wl_sem.at[slot])

    def w_remote(slot):
        return remote(
            columns(slot, 1), woth.at[slot], w_send.at[slot], w_recv.at[slot], partner
        )

    def nkv_remote():
        return (
            remote(nk_hbm, nk.at[half], nkv_send.at[0], nkv_recv.at[0], partner),
            remote(nv_hbm, nv.at[half], nkv_send.at[1], nkv_recv.at[1], partner),
        )

    def attended_remote(s):
        return remote(aown.at[s], aoth.at[s], a_send.at[s], a_recv.at[s], partner)

    def first_remote(s):
        return (
            remote(pbuf.at[s, SLOT[2, 0], 0], r1.at[s, 0], r1_send.at[s, 0], r1_recv.at[s, 0], up),
            remote(pbuf.at[s, SLOT[2, 1], 0], r1.at[s, 1], r1_send.at[s, 1], r1_recv.at[s, 1], down),
        )

    def direct_remote(s):
        return (
            remote(pbuf.at[s, SLOT[1, 1], 0], r2.at[s, 1], r2_send.at[s, 1], r2_recv.at[s, 1], up),
            remote(pbuf.at[s, SLOT[3, 0], 0], r2.at[s, 2], r2_send.at[s, 2], r2_recv.at[s, 2], down),
        )

    def forward_remote(s):
        return (
            remote(fbuf.at[s, 0], r2.at[s, 0], r2_send.at[s, 0], r2_recv.at[s, 0], up),
            remote(fbuf.at[s, 1], r2.at[s, 3], r2_send.at[s, 3], r2_recv.at[s, 3], down),
        )

    def x_remote(s):
        return remote(xbuf.at[s], rx.at[s], x_send.at[s], x_recv.at[s], across)

    def x_first_remote(s, dy):
        return remote(
            pbuf.at[s, SLOT[dy, 1], 1], rxx.at[s, dy], xx_send.at[s, dy], xx_recv.at[s, dy], across
        )

    def low_high(ref, s, i, high):
        return ref.at[s, i, pl.ds(high * TALL, TALL)]

    def y_first_remote(s):
        return (
            remote(low_high(cbuf, s, 0, 0), q1.at[s, 0], q1_send.at[s, 0], q1_recv.at[s, 0], up),
            remote(low_high(cbuf, s, 0, 1), q1.at[s, 1], q1_send.at[s, 1], q1_recv.at[s, 1], down),
        )

    def y_direct_remote(s):
        return (
            remote(
                low_high(cbuf, s, 1, 1), low_high(q2, s, 0, 1),
                q2_send.at[s, 1], q2_recv.at[s, 1], up,
            ),
            remote(
                low_high(cbuf, s, 2, 0), low_high(q2, s, 1, 0),
                q2_send.at[s, 2], q2_recv.at[s, 2], down,
            ),
        )

    def y_forward_remote(s):
        return (
            remote(gbuf.at[s, 0], low_high(q2, s, 0, 0), q2_send.at[s, 0], q2_recv.at[s, 0], up),
            remote(gbuf.at[s, 1], low_high(q2, s, 1, 1), q2_send.at[s, 3], q2_recv.at[s, 3], down),
        )

    others = [(dy, dx, dc) for dy in range(4) for dx in range(2) for dc in range(2)][1:]

    def square_remote(i):
        return remote(ss, ssr.at[i], ss_send.at[i], ss_recv.at[i], peer(*others[i]))

    load = (
        pltpu.make_async_copy(q_hbm, q_v, load_sem.at[0]),
        pltpu.make_async_copy(nk_hbm, nk.at[half], load_sem.at[1]),
        pltpu.make_async_copy(nv_hbm, nv.at[half], load_sem.at[2]),
        pltpu.make_async_copy(res_hbm, res_v, load_sem.at[3]),
    )

    barrier = pltpu.get_barrier_semaphore()
    for dev in (partner, up, down, far, across):
        pl.semaphore_signal(barrier, inc=1, device_id={"tp": dev}, device_id_type=MESH)
    load[0].start()
    for copy in kv_local(0):
        copy.start()
    load[1].start()
    load[2].start()
    pl.semaphore_wait(barrier, 5)

    for copy in kv_remote(0) + nkv_remote():
        copy.start()
    for slot in range(4):
        w_remote(slot).start()
    for s in range(1, SEQS):
        for copy in kv_local(s):
            copy.start()
    for slot in range(8):
        w_local(slot).start()
    load[3].start()

    def rows_of(s, chunk):
        part = q_v[pl.ds(pl.multiple_of(s * SPAN, SPAN), SPAN), :]
        heads = range(chunk * HEADS, (chunk + 1) * HEADS)
        return jnp.concatenate([part[:, h * HD : (h + 1) * HD] for h in heads], axis=0)

    def chunk_rows(chunk):
        return slice(chunk * ROWS, (chunk + 1) * ROWS)

    def own_half(s):
        for copy in kv_local(s):
            copy.wait()
        upcoming = dot_t(rows_of(s, 0), kown[s])
        for chunk in range(CHUNKS):
            scores = upcoming
            if chunk + 1 < CHUNKS:
                upcoming = dot_t(rows_of(s, chunk + 1), kown[s])
            rows = chunk_rows(chunk)
            peak = jnp.max(scores, axis=1, keepdims=True)
            weights = jnp.exp2((scores - peak) * SCALE).astype(BF16)
            acc_ref[rows, :] = dot(weights, with_ones(vown[s]))
            m_ref[rows, :] = jnp.broadcast_to(peak, (ROWS, HD))

    def other_half(s):
        for copy in kv_remote(s):
            copy.wait_recv()
        tokens = pl.ds(pl.multiple_of(s * SPAN, SPAN), SPAN)

        def scores_of(chunk):
            q = rows_of(s, chunk)
            recent = dot(q, nk[:, tokens])
            row = lax.rem(lax.broadcasted_iota(jnp.int32, recent.shape, 0), SPAN)
            col = lax.broadcasted_iota(jnp.int32, recent.shape, 1)
            return dot_t(q, koth[s]), jnp.where(row >= col, recent, -jnp.inf)

        upcoming = scores_of(0)
        for chunk in range(CHUNKS):
            scores, recent = upcoming
            if chunk + 1 < CHUNKS:
                upcoming = scores_of(chunk + 1)
            rows = chunk_rows(chunk)
            old = m_ref[rows, :1]
            peak = jnp.maximum(
                jnp.max(scores, axis=1, keepdims=True), jnp.max(recent, axis=1, keepdims=True)
            )
            peak = jnp.maximum(peak, old)
            weights = jnp.exp2((scores - peak) * SCALE).astype(BF16)
            recent_weights = jnp.exp2((recent - peak) * SCALE).astype(BF16)
            mixed = acc_ref[rows, :] * jnp.exp2((old - peak) * SCALE)
            mixed = mixed + dot(weights, with_ones(voth[s]))
            mixed = mixed + dot_t(recent_weights, with_ones(nv[:, tokens], 0))
            result = (mixed[:, :HD] / mixed[:, HD:]).astype(BF16)
            for i in range(HEADS):
                h = chunk * HEADS + i
                aown[s, :, h * HD : (h + 1) * HD] = result[i * SPAN : (i + 1) * SPAN, :]

    def project(s):
        attended_remote(s).wait_recv()
        for slot, (dy, dx) in enumerate(ORDER):
            @pl.when(s == 0)
            def _():
                w_local(slot).wait()
                w_remote(slot).wait_recv()

            block = (dot(aown[s], wown[slot]) + dot(aoth[s], woth[slot])).astype(BF16)
            pbuf[s, slot, 0] = block[:, :WIDE]
            pbuf[s, slot, 1] = block[:, WIDE:]
            if dx == 1:
                x_first_remote(s, dy).start()
            if dy == 2:
                first_remote(s)[dx].start()
            elif (dy, dx) == (1, 1):
                direct_remote(s)[0].start()
            elif (dy, dx) == (3, 0):
                direct_remote(s)[1].start()

    def wide(ref):
        return ref.astype(F32)

    def forward(s):
        for i, slot in enumerate((SLOT[1, 0], SLOT[3, 1])):
            first_remote(s)[i].wait_recv()
            fbuf[s, i] = (wide(r1[s, i]) + wide(pbuf[s, slot, 0])).astype(BF16)
            forward_remote(s)[i].start()

    def send_across(s):
        direct_remote(s)[0].wait_recv()
        forward_remote(s)[1].wait_recv()
        total = wide(pbuf[s, SLOT[0, 1], 0]) + wide(r2[s, 1]) + wide(r2[s, 3])
        xbuf[s] = total.astype(BF16)
        x_remote(s).start()

    def sum_across(s):
        for i, dy in enumerate((2, 1, 3)):
            x_first_remote(s, dy).wait_recv()
            cbuf[s, i] = (wide(pbuf[s, SLOT[dy, 0], 1]) + wide(rxx[s, dy])).astype(BF16)
            if i == 0:
                for copy in y_first_remote(s):
                    copy.start()
            else:
                y_direct_remote(s)[i - 1].start()

    def y_forward(s):
        for i in range(2):
            y_first_remote(s)[i].wait_recv()
            kept = cbuf[s, 1 + i, i * TALL : (i + 1) * TALL, :]
            gbuf[s, i] = (wide(q1[s, i]) + wide(kept)).astype(BF16)
            y_forward_remote(s)[i].start()

    def finish(s):
        tokens = pl.ds(pl.multiple_of(s * SPAN, SPAN), SPAN)
        direct_remote(s)[1].wait_recv()
        forward_remote(s)[0].wait_recv()
        x_remote(s).wait_recv()
        left = wide(pbuf[s, SLOT[0, 0], 0]) + wide(r2[s, 0]) + wide(r2[s, 2]) + wide(rx[s])
        left = left + wide(res_v[tokens, :WIDE])
        hid[s, :, :WIDE] = left
        x_first_remote(s, 0).wait_recv()
        for copy in y_direct_remote(s) + y_forward_remote(s):
            copy.wait_recv()
        right = wide(pbuf[s, SLOT[0, 0], 1]) + wide(rxx[s, 0]) + wide(q2[s, 0]) + wide(q2[s, 1])
        right = right + wide(res_v[tokens, WIDE:])
        hid[s, :, WIDE:] = right
        column = jnp.sum(left * left + right * right, axis=1, keepdims=True)
        ss[s : s + 1, :] = jnp.transpose(jnp.broadcast_to(column, (SPAN, SPAN)))[:1, :]

    load[0].wait()

    def sequence(s, carry):
        own_half(s)

        @pl.when(s >= 1)
        def _():
            forward(s - 1)

        @pl.when(s >= 2)
        def _():
            y_forward(s - 2)
            send_across(s - 2)

        @pl.when(s == 0)
        def _():
            for copy in load[1:3]:
                copy.wait()
            for copy in nkv_remote():
                copy.wait_recv()

        other_half(s)
        attended_remote(s).start()

        @pl.when(s == 0)
        def _():
            for slot in range(4, 8):
                w_remote(slot).start()

        @pl.when(s < SEQS - 1)
        def _():
            for copy in kv_remote(s + 1):
                copy.start()

        @pl.when(s >= 1)
        def _():
            sum_across(s - 1)

        project(s)
        return carry

    lax.fori_loop(0, SEQS, sequence, 0)

    load[3].wait()
    ss[...] = jnp.zeros_like(ss)
    y_forward(SEQS - 2)
    send_across(SEQS - 2)
    finish(0)
    finish(1)
    forward(SEQS - 1)
    sum_across(SEQS - 1)
    finish(2)
    send_across(SEQS - 1)
    y_forward(SEQS - 1)
    finish(3)

    for i in range(15):
        square_remote(i).start()

    for copy in nkv_remote():
        copy.wait_send()
    for slot in range(8):
        w_remote(slot).wait_send()

    def drain(s, carry):
        for copy in kv_remote(s) + first_remote(s) + direct_remote(s) + forward_remote(s):
            copy.wait_send()
        for copy in y_first_remote(s) + y_direct_remote(s) + y_forward_remote(s):
            copy.wait_send()
        for dy in range(4):
            x_first_remote(s, dy).wait_send()
        attended_remote(s).wait_send()
        x_remote(s).wait_send()
        return carry

    lax.fori_loop(0, SEQS, drain, 0)

    lines = gain_ref[...].astype(F32)
    gain = jnp.concatenate([lines[i : i + 1, :] for i in range(4)], axis=1)
    for i in range(15):
        square_remote(i).wait_recv()
    squares = ss[...]
    for i in range(15):
        squares = squares + ssr[i]
    rows = lax.rsqrt(squares * (1.0 / D) + EPSILON)
    for s in range(SEQS):
        column = jnp.transpose(jnp.broadcast_to(rows[s : s + 1, :], (SPAN, SPAN)))[:, :1]
        out_ref[s * SPAN : (s + 1) * SPAN, :] = (hid[s] * column * gain).astype(BF16)
    for i in range(15):
        square_remote(i).wait_send()


def per_device(queries, new_keys, new_values, cache_keys, cache_values, out_weight, residual, gain):
    any_spec = pl.BlockSpec(memory_space=pl.ANY)
    vmem_spec = pl.BlockSpec(memory_space=pltpu.VMEM)
    dma = pltpu.SemaphoreType.DMA
    block = (SPAN, WIDE)
    return pl.pallas_call(
        kernel,
        name="attend",
        out_shape=pltpu.VMEM((SEQS * SPAN, COLS), BF16),
        in_specs=[any_spec] * 7 + [vmem_spec],
        out_specs=vmem_spec,
        scratch_shapes=[
            pltpu.VMEM((SEQS * SPAN, 4 * HD), BF16),
            *[pltpu.VMEM((SEQS, HALF, HD), BF16)] * 4,
            *[pltpu.VMEM((HD, SEQS * SPAN), BF16)] * 2,
            *[pltpu.VMEM((8, COLS, COLS), BF16)] * 2,
            pltpu.VMEM((4 * SPAN, HD), F32),
            pltpu.VMEM((4 * SPAN, 2 * HD), F32),
            *[pltpu.VMEM((SEQS, SPAN, COLS), BF16)] * 2,
            pltpu.VMEM((SEQS, 8, 2, *block), BF16),
            pltpu.VMEM((SEQS, 2, *block), BF16),
            pltpu.VMEM((SEQS, *block), BF16),
            pltpu.VMEM((SEQS, 2, *block), BF16),
            pltpu.VMEM((SEQS, 4, *block), BF16),
            pltpu.VMEM((SEQS, *block), BF16),
            pltpu.VMEM((SEQS, 4, *block), BF16),
            pltpu.VMEM((SEQS, 3, *block), BF16),
            pltpu.VMEM((SEQS, 2, TALL, WIDE), BF16),
            pltpu.VMEM((SEQS, 2, TALL, WIDE), BF16),
            pltpu.VMEM((SEQS, 2, *block), BF16),
            pltpu.VMEM((SEQS, SPAN, COLS), F32),
            pltpu.VMEM((SEQS * SPAN, COLS), BF16),
            pltpu.VMEM((8, SPAN), F32),
            pltpu.VMEM((15, 8, SPAN), F32),
            dma((4,)), dma((SEQS, 2)), dma((8,)),
            dma((SEQS, 2)), dma((SEQS, 2)), dma((2,)), dma((2,)),
            dma((8,)), dma((8,)), dma((SEQS,)), dma((SEQS,)),
            dma((SEQS, 2)), dma((SEQS, 2)), dma((SEQS, 4)), dma((SEQS, 4)),
            dma((SEQS,)), dma((SEQS,)), dma((SEQS, 4)), dma((SEQS, 4)),
            dma((SEQS, 2)), dma((SEQS, 2)), dma((SEQS, 4)), dma((SEQS, 4)),
            dma((15,)), dma((15,)),
        ],
        compiler_params=pltpu.CompilerParams(
            collective_id=0, has_side_effects=True, vmem_limit_bytes=60 * 2**20
        ),
    )(
        queries, new_keys.T, new_values.T, cache_keys, cache_values, out_weight, residual,
        gain.reshape(4, 128),
    )


def solution(mesh):
    in_specs = (
        P("dp", "tp"),
        P("dp", "tp"),
        P("dp", "tp"),
        P("dp", "tp", None),
        P("dp", "tp", None),
        P("tp", None),
        P("dp", "tp"),
        P("tp"),
    )
    return jax.shard_map(
        per_device, mesh=mesh, in_specs=in_specs, out_specs=P("dp", "tp"), check_vma=False
    )
```

```python
import jax
import jax.numpy as jnp
from jax import lax
from jax.experimental import pallas as pl
from jax.experimental.pallas import tpu as pltpu
from jax.sharding import PartitionSpec as P

D = 8192
HD = 128
SPAN = 128
SEQS = 4
HALF = 2048
COLS = 512
EPSILON = 1e-05
SCALE = HD**-0.5 * 1.4426950408889634

MESH = pl.DeviceIdType.MESH
F32 = jnp.float32
BF16 = jnp.bfloat16

ORDER = ((2, 1), (2, 0), (1, 1), (3, 0), (3, 1), (0, 1), (1, 0), (0, 0))
SLOT = {key: slot for slot, key in enumerate(ORDER)}
WIDE = COLS // 2
TALL = SPAN // 2
LAST = SEQS - 1
GROUPS = ((0, 1, 2, 3), (4, 5, 6, 7))
HEADS = 2
ROWS = HEADS * SPAN
CHUNKS = 4 // HEADS


def dot_t(a, b):
    return lax.dot_general(a, b, (((1,), (1,)), ((), ())), preferred_element_type=F32)


def dot(a, b):
    return jnp.dot(a, b, preferred_element_type=F32)


def with_ones(v, axis=1):
    return jnp.concatenate([v, jnp.ones_like(v)], axis=axis)


def kernel(
    q_hbm, nk_hbm, nv_hbm, ck_hbm, cv_hbm, w_hbm, res_hbm, gain_ref, out_ref,
    q_v, kown, vown, koth, voth, nk, nv, wown, wsend, m_ref, acc_ref, aown, psend, precv,
    pbuf, fbuf, xbuf, r1, r2, rx, rxx, cbuf, gbuf, q1, q2, q3,
    hid, res_v, ss, ssr,
    load_sem, kvl_sem, wl_sem, sent, kv_recv, nkv_recv, p_recv,
    r1_recv, r2_recv, x_recv, xx_recv, q1_recv, q2_recv, q3_recv, ss_recv,
):
    me = lax.axis_index("tp")
    core = lax.rem(me, 2)
    xh = lax.rem(lax.div(me, 2), 2)
    y = lax.div(me, 4)
    half = pl.ds(pl.multiple_of(core * (HD // 2), HD // 2), HD // 2)

    def peer(dy, dx, dc):
        py = lax.rem(y + dy, 4)
        px = lax.rem(xh + dx, 2)
        pc = lax.rem(core + dc, 2)
        return (py * 2 + px) * 2 + pc

    partner = peer(0, 0, 1)
    up, down, far, across = peer(1, 0, 0), peer(3, 0, 0), peer(2, 0, 0), peer(0, 1, 0)

    def remote(src, dst, send, recv, dev):
        return pltpu.make_async_remote_copy(
            src_ref=src, dst_ref=dst, send_sem=send, recv_sem=recv,
            device_id={"tp": dev}, device_id_type=MESH,
        )

    def kv_local(s):
        return (
            pltpu.make_async_copy(ck_hbm.at[s], kown.at[s], kvl_sem.at[s, 0]),
            pltpu.make_async_copy(cv_hbm.at[s], vown.at[s], kvl_sem.at[s, 1]),
        )

    def kv_remote(s):
        return (
            remote(kown.at[s], koth.at[s], sent.at[0], kv_recv.at[s, 0], partner),
            remote(vown.at[s], voth.at[s], sent.at[1], kv_recv.at[s, 1], partner),
        )

    def columns(slot, dc):
        dy, dx = ORDER[slot]
        start = peer(dy, dx, dc) * COLS
        return w_hbm.at[:, pl.ds(pl.multiple_of(start, COLS), COLS)]

    def w_local(slot):
        return pltpu.make_async_copy(columns(slot, 0), wown.at[slot], wl_sem.at[0])

    def w_staged(slot):
        return pltpu.make_async_copy(columns(slot, 1), wsend.at[slot], wl_sem.at[1])

    def nkv_remote():
        return (
            remote(nk.at[half], nk.at[half], sent.at[2], nkv_recv.at[0], partner),
            remote(nv.at[half], nv.at[half], sent.at[3], nkv_recv.at[1], partner),
        )

    def wait_bytes(ref, sem):
        pltpu.make_async_copy(ref, ref, sem).wait()

    def share_remote(s, slot):
        return remote(
            psend.at[s, slot], precv.at[s, slot], sent.at[4], p_recv.at[s, slot // 4], partner
        )

    def first_remote(s):
        return (
            remote(pbuf.at[s, SLOT[2, 0], 0], r1.at[s, 0], sent.at[5], r1_recv.at[s, 0], up),
            remote(pbuf.at[s, SLOT[2, 1], 0], r1.at[s, 1], sent.at[5], r1_recv.at[s, 1], down),
        )

    def direct_remote(s):
        return (
            remote(pbuf.at[s, SLOT[1, 1], 0], r2.at[s, 1], sent.at[5], r2_recv.at[s, 1], up),
            remote(pbuf.at[s, SLOT[3, 0], 0], r2.at[s, 2], sent.at[5], r2_recv.at[s, 2], down),
        )

    def forward_remote(s):
        return (
            remote(fbuf.at[s, 0], r2.at[s, 0], sent.at[6], r2_recv.at[s, 0], up),
            remote(fbuf.at[s, 1], r2.at[s, 3], sent.at[6], r2_recv.at[s, 3], down),
        )

    def x_remote(s):
        return remote(xbuf.at[s], rx.at[s], sent.at[7], x_recv.at[s], across)

    def x_first_remote(s, dy):
        return remote(
            pbuf.at[s, SLOT[dy, 1], 1], rxx.at[s, dy], sent.at[5], xx_recv.at[s, dy], across
        )

    def y_last_remote():
        return tuple(
            remote(cbuf.at[LAST, i], q3.at[i], sent.at[8], q3_recv.at[i], dev)
            for i, dev in enumerate((far, up, down))
        )

    def tall(ref, s, i, low):
        return ref.at[s, i, pl.ds(low * TALL, TALL)]

    def y_first_remote(s):
        return (
            remote(tall(cbuf, s, 0, 0), q1.at[s, 0], sent.at[10], q1_recv.at[s, 0], up),
            remote(tall(cbuf, s, 0, 1), q1.at[s, 1], sent.at[10], q1_recv.at[s, 1], down),
        )

    def y_direct_remote(s):
        return (
            remote(tall(cbuf, s, 1, 1), tall(q2, s, 0, 1), sent.at[11], q2_recv.at[s, 1], up),
            remote(tall(cbuf, s, 2, 0), tall(q2, s, 1, 0), sent.at[11], q2_recv.at[s, 2], down),
        )

    def y_forward_remote(s):
        return (
            remote(gbuf.at[s, 0], tall(q2, s, 0, 0), sent.at[12], q2_recv.at[s, 0], up),
            remote(gbuf.at[s, 1], tall(q2, s, 1, 1), sent.at[12], q2_recv.at[s, 3], down),
        )

    others = [(dy, dx, dc) for dy in range(4) for dx in range(2) for dc in range(2)][1:]

    def square_remote(i):
        return remote(ss, ssr.at[i], sent.at[9], ss_recv, peer(*others[i]))

    load = (
        pltpu.make_async_copy(q_hbm, q_v, load_sem.at[0]),
        pltpu.make_async_copy(nk_hbm, nk.at[half], load_sem.at[1]),
        pltpu.make_async_copy(nv_hbm, nv.at[half], load_sem.at[2]),
        pltpu.make_async_copy(res_hbm, res_v, load_sem.at[3]),
    )

    barrier = pltpu.get_barrier_semaphore()
    for dev in (partner, up, down, far, across):
        pl.semaphore_signal(barrier, inc=1, device_id={"tp": dev}, device_id_type=MESH)
    first_load = kv_local(0) + load[1:3] + load[:1]
    for copy in first_load:
        copy.start()
    for copy in first_load:
        copy.wait()
    for slot in range(8):
        w_staged(slot).start()
    pl.semaphore_wait(barrier, 5)

    for pair in zip(kv_remote(0), nkv_remote()):
        for copy in pair:
            copy.start()
    for copy in kv_local(1):
        copy.start()
    for slot in range(8):
        w_local(slot).start()
    for s in range(2, SEQS):
        for copy in kv_local(s):
            copy.start()
    load[3].start()

    def rows_of(s, chunk):
        part = q_v[pl.ds(pl.multiple_of(s * SPAN, SPAN), SPAN), :]
        heads = range(chunk * HEADS, (chunk + 1) * HEADS)
        return jnp.concatenate([part[:, h * HD : (h + 1) * HD] for h in heads], axis=0)

    def chunk_rows(chunk):
        return slice(chunk * ROWS, (chunk + 1) * ROWS)

    def own_half(s):
        upcoming = dot_t(rows_of(s, 0), kown[s])
        for chunk in range(CHUNKS):
            scores = upcoming
            if chunk + 1 < CHUNKS:
                upcoming = dot_t(rows_of(s, chunk + 1), kown[s])
            rows = chunk_rows(chunk)
            peak = jnp.max(scores, axis=1, keepdims=True)
            weights = jnp.exp2((scores - peak) * SCALE).astype(BF16)
            acc_ref[rows, :] = dot(weights, with_ones(vown[s]))
            m_ref[rows, :] = jnp.broadcast_to(peak, (ROWS, HD))

    def other_half(s):
        kv_remote(s)[0].wait_recv()
        tokens = pl.ds(pl.multiple_of(s * SPAN, SPAN), SPAN)

        def scores_of(chunk):
            q = rows_of(s, chunk)
            recent = dot(q, nk[:, tokens])
            row = lax.rem(lax.broadcasted_iota(jnp.int32, recent.shape, 0), SPAN)
            col = lax.broadcasted_iota(jnp.int32, recent.shape, 1)
            return dot_t(q, koth[s]), jnp.where(row >= col, recent, -jnp.inf)

        upcoming = scores_of(0)
        for chunk in range(CHUNKS):
            scores, recent = upcoming
            if chunk + 1 < CHUNKS:
                upcoming = scores_of(chunk + 1)
            rows = chunk_rows(chunk)
            old = m_ref[rows, :1]
            peak = jnp.maximum(
                jnp.max(scores, axis=1, keepdims=True), jnp.max(recent, axis=1, keepdims=True)
            )
            peak = jnp.maximum(peak, old)
            weights = jnp.exp2((scores - peak) * SCALE).astype(BF16)
            recent_weights = jnp.exp2((recent - peak) * SCALE).astype(BF16)
            mixed = acc_ref[rows, :] * jnp.exp2((old - peak) * SCALE)
            if chunk == 0:
                kv_remote(s)[1].wait_recv()
            mixed = mixed + dot(weights, with_ones(voth[s]))
            mixed = mixed + dot_t(recent_weights, with_ones(nv[:, tokens], 0))
            result = (mixed[:, :HD] / mixed[:, HD:]).astype(BF16)
            for i in range(HEADS):
                h = chunk * HEADS + i
                aown[s, :, h * HD : (h + 1) * HD] = result[i * SPAN : (i + 1) * SPAN, :]

    def wide(ref):
        return ref.astype(F32)

    def share(s):
        for group in GROUPS:
            for slot in group:
                psend[s, slot] = dot(aown[s], wsend[slot]).astype(BF16)
            for slot in group:
                share_remote(s, slot).start()

    def project(s):
        for group in GROUPS:
            blocks = [dot(aown[s], wown[slot]) for slot in group]
            wait_bytes(precv.at[s, pl.ds(group[0], 4)], p_recv.at[s, group[0] // 4])
            for slot, block in zip(group, blocks):
                block = (block + wide(precv[s, slot])).astype(BF16)
                pbuf[s, slot, 0] = block[:, :WIDE]
                pbuf[s, slot, 1] = block[:, WIDE:]
            for slot in group:
                dy, dx = ORDER[slot]
                if dx == 1:
                    x_first_remote(s, dy).start()
                if dy == 2:
                    first_remote(s)[dx].start()
                elif (dy, dx) == (1, 1):
                    direct_remote(s)[0].start()
                elif (dy, dx) == (3, 0):
                    direct_remote(s)[1].start()

    def forward(s):
        for i, slot in enumerate((SLOT[1, 0], SLOT[3, 1])):
            first_remote(s)[i].wait_recv()
            fbuf[s, i] = (wide(r1[s, i]) + wide(pbuf[s, slot, 0])).astype(BF16)
            forward_remote(s)[i].start()

    def send_across(s):
        direct_remote(s)[0].wait_recv()
        forward_remote(s)[1].wait_recv()
        total = wide(pbuf[s, SLOT[0, 1], 0]) + wide(r2[s, 1]) + wide(r2[s, 3])
        xbuf[s] = total.astype(BF16)
        x_remote(s).start()

    def sum_across(s):
        for i, dy in enumerate((2, 1, 3)):
            x_first_remote(s, dy).wait_recv()
            cbuf[s, i] = (wide(pbuf[s, SLOT[dy, 0], 1]) + wide(rxx[s, dy])).astype(BF16)
            if isinstance(s, int):
                y_last_remote()[i].start()
            elif i == 0:
                for copy in y_first_remote(s):
                    copy.start()
            else:
                y_direct_remote(s)[i - 1].start()

    def y_forward(s):
        for i in range(2):
            y_first_remote(s)[i].wait_recv()
            kept = wide(cbuf[s, 1 + i, i * TALL : (i + 1) * TALL, :])
            gbuf[s, i] = (wide(q1[s, i]) + kept).astype(BF16)
            y_forward_remote(s)[i].start()

    def finish(s):
        tokens = pl.ds(pl.multiple_of(s * SPAN, SPAN), SPAN)
        x_first_remote(s, 0).wait_recv()
        right = wide(pbuf[s, SLOT[0, 0], 1]) + wide(rxx[s, 0])
        if s == LAST:
            for i, copy in enumerate(y_last_remote()):
                copy.wait_recv()
                right = right + wide(q3[i])
        else:
            for copy in y_direct_remote(s) + y_forward_remote(s):
                copy.wait_recv()
            right = right + wide(q2[s, 0]) + wide(q2[s, 1])
        right = right + wide(res_v[tokens, WIDE:])
        hid[s, :, WIDE:] = right
        direct_remote(s)[1].wait_recv()
        forward_remote(s)[0].wait_recv()
        left = wide(pbuf[s, SLOT[0, 0], 0]) + wide(r2[s, 0]) + wide(r2[s, 2])
        left = left + wide(res_v[tokens, :WIDE])
        x_remote(s).wait_recv()
        left = left + wide(rx[s])
        hid[s, :, :WIDE] = left
        column = jnp.sum(left * left + right * right, axis=1, keepdims=True)
        ss[s : s + 1, :] = jnp.transpose(jnp.broadcast_to(column, (SPAN, SPAN)))[:1, :]

    own_half(0)
    for copy in kv_local(1):
        copy.wait()
    for copy in kv_remote(1):
        copy.start()
    for copy in nkv_remote():
        copy.wait_recv()

    def sequence(s, carry):
        other_half(s)

        @pl.when(s == 0)
        def _():
            wait_bytes(wown, wl_sem.at[0])
            wait_bytes(wsend, wl_sem.at[1])

        share(s)

        @pl.when(s < SEQS - 2)
        def _():
            for copy in kv_local(s + 2):
                copy.wait()
            for copy in kv_remote(s + 2):
                copy.start()

        @pl.when(s >= 1)
        def _():
            forward(s - 1)

        @pl.when(s >= 2)
        def _():
            send_across(s - 2)
            y_forward(s - 2)

        @pl.when((s >= 1) & (s < SEQS - 1))
        def _():
            own_half(s + 1)

        project(s)

        @pl.when(s == 0)
        def _():
            own_half(1)

        @pl.when(s >= 1)
        def _():
            sum_across(s - 1)

        return carry

    lax.fori_loop(0, SEQS, sequence, 0)

    load[3].wait()
    ss[...] = jnp.zeros_like(ss)
    finish(0)
    forward(LAST)
    send_across(LAST - 1)
    y_forward(LAST - 1)
    finish(1)
    sum_across(SEQS - 1)
    send_across(SEQS - 1)
    finish(2)
    finish(3)

    for i in range(15):
        square_remote(i).start()

    sources = (
        kown, vown, nk.at[half], nv.at[half], psend, pbuf.at[:, pl.ds(0, 4)], fbuf, xbuf,
        cbuf.at[LAST], ssr, q1, q1, gbuf,
    )
    for i, ref in enumerate(sources):
        if ref is not ssr:
            wait_bytes(ref, sent.at[i])

    lines = gain_ref[...].astype(F32)
    gain = jnp.concatenate([lines[i : i + 1, :] for i in range(4)], axis=1)
    wait_bytes(ssr, ss_recv)
    squares = ss[...]
    for i in range(15):
        squares = squares + ssr[i]
    rows = lax.rsqrt(squares * (1.0 / D) + EPSILON)
    for s in range(SEQS):
        column = jnp.transpose(jnp.broadcast_to(rows[s : s + 1, :], (SPAN, SPAN)))[:, :1]
        out_ref[s * SPAN : (s + 1) * SPAN, :] = (hid[s] * column * gain).astype(BF16)
    wait_bytes(ssr, sent.at[9])


def per_device(queries, new_keys, new_values, cache_keys, cache_values, out_weight, residual, gain):
    any_spec = pl.BlockSpec(memory_space=pl.ANY)
    vmem_spec = pl.BlockSpec(memory_space=pltpu.VMEM)
    dma = pltpu.SemaphoreType.DMA
    block = (SPAN, WIDE)
    return pl.pallas_call(
        kernel,
        name="attend",
        out_shape=pltpu.VMEM((SEQS * SPAN, COLS), BF16),
        in_specs=[any_spec] * 7 + [vmem_spec],
        out_specs=vmem_spec,
        scratch_shapes=[
            pltpu.VMEM((SEQS * SPAN, 4 * HD), BF16),
            *[pltpu.VMEM((SEQS, HALF, HD), BF16)] * 4,
            *[pltpu.VMEM((HD, SEQS * SPAN), BF16)] * 2,
            *[pltpu.VMEM((8, COLS, COLS), BF16)] * 2,
            pltpu.VMEM((4 * SPAN, HD), F32),
            pltpu.VMEM((4 * SPAN, 2 * HD), F32),
            pltpu.VMEM((SEQS, SPAN, COLS), BF16),
            *[pltpu.VMEM((SEQS, 8, SPAN, COLS), BF16)] * 2,
            pltpu.VMEM((SEQS, 8, 2, *block), BF16),
            pltpu.VMEM((SEQS, 2, *block), BF16),
            pltpu.VMEM((SEQS, *block), BF16),
            pltpu.VMEM((SEQS, 2, *block), BF16),
            pltpu.VMEM((SEQS, 4, *block), BF16),
            pltpu.VMEM((SEQS, *block), BF16),
            pltpu.VMEM((SEQS, 4, *block), BF16),
            pltpu.VMEM((SEQS, 3, *block), BF16),
            *[pltpu.VMEM((LAST, 2, TALL, WIDE), BF16)] * 2,
            pltpu.VMEM((LAST, 2, *block), BF16),
            pltpu.VMEM((3, *block), BF16),
            pltpu.VMEM((SEQS, SPAN, COLS), F32),
            pltpu.VMEM((SEQS * SPAN, COLS), BF16),
            pltpu.VMEM((8, SPAN), F32),
            pltpu.VMEM((15, 8, SPAN), F32),
            dma((4,)), dma((SEQS, 2)), dma((2,)), dma((13,)), dma((SEQS, 2)), dma((2,)),
            dma((SEQS, 2)), dma((SEQS, 2)), dma((SEQS, 4)), dma((SEQS,)), dma((SEQS, 4)),
            dma((LAST, 2)), dma((LAST, 4)), dma((3,)), dma,
        ],
        compiler_params=pltpu.CompilerParams(
            collective_id=0, has_side_effects=True, vmem_limit_bytes=60 * 2**20
        ),
    )(
        queries, new_keys.T, new_values.T, cache_keys, cache_values, out_weight, residual,
        gain.reshape(4, 128),
    )


def solution(mesh):
    in_specs = (
        P("dp", "tp"),
        P("dp", "tp"),
        P("dp", "tp"),
        P("dp", "tp", None),
        P("dp", "tp", None),
        P("tp", None),
        P("dp", "tp"),
        P("tp"),
    )
    return jax.shard_map(
        per_device, mesh=mesh, in_specs=in_specs, out_specs=P("dp", "tp"), check_vma=False
    )
```

```python
import jax
import jax.numpy as jnp
from jax import lax
from jax.experimental import pallas as pl
from jax.experimental.pallas import tpu as pltpu
from jax.sharding import PartitionSpec as P

D = 8192
HD = 128
SPAN = 128
SEQS = 4
HALF = 2048
COLS = 512
EPSILON = 1e-05
SCALE = HD**-0.5 * 1.4426950408889634

MESH = pl.DeviceIdType.MESH
F32 = jnp.float32
BF16 = jnp.bfloat16

ORDER = ((2, 1), (2, 0), (1, 1), (3, 0), (3, 1), (0, 1), (1, 0), (0, 0))
SLOT = {key: slot for slot, key in enumerate(ORDER)}
WIDE = COLS // 2
TALL = SPAN // 2
LAST = SEQS - 1
GROUPS = ((0, 1, 2, 3), (4, 5, 6, 7))
HEADS = 2
ROWS = HEADS * SPAN
CHUNKS = 4 // HEADS


def dot_t(a, b):
    return lax.dot_general(a, b, (((1,), (1,)), ((), ())), preferred_element_type=F32)


def dot(a, b):
    return jnp.dot(a, b, preferred_element_type=F32)


def with_ones(v, axis=1):
    return jnp.concatenate([v, jnp.ones_like(v)], axis=axis)


def kernel(
    q_hbm, nk_hbm, nv_hbm, ck_hbm, cv_hbm, w_hbm, res_hbm, gain_ref, out_ref,
    q_v, kown, vown, koth, voth, nk, nv, wown, wsend, m_ref, acc_ref, aown, psend, precv,
    pbuf, fbuf, xbuf, r1, r2, rx, rxx, cbuf, gbuf, q1, q2, q3,
    hid, res_v, ss, ssr,
    load_sem, kvl_sem, wl_sem, sent, kv_recv, nkv_recv, p_recv,
    r1_recv, r2_recv, x_recv, xx_recv, q1_recv, q2_recv, q3_recv, ss_recv,
):
    me = lax.axis_index("tp")
    core = lax.rem(me, 2)
    xh = lax.rem(lax.div(me, 2), 2)
    y = lax.div(me, 4)
    half = pl.ds(pl.multiple_of(core * (HD // 2), HD // 2), HD // 2)

    def peer(dy, dx, dc):
        py = lax.rem(y + dy, 4)
        px = lax.rem(xh + dx, 2)
        pc = lax.rem(core + dc, 2)
        return (py * 2 + px) * 2 + pc

    partner = peer(0, 0, 1)
    up, down, far, across = peer(1, 0, 0), peer(3, 0, 0), peer(2, 0, 0), peer(0, 1, 0)

    def remote(src, dst, send, recv, dev):
        return pltpu.make_async_remote_copy(
            src_ref=src, dst_ref=dst, send_sem=send, recv_sem=recv,
            device_id={"tp": dev}, device_id_type=MESH,
        )

    def kv_local(s):
        return (
            pltpu.make_async_copy(ck_hbm.at[s], kown.at[s], kvl_sem.at[s, 0]),
            pltpu.make_async_copy(cv_hbm.at[s], vown.at[s], kvl_sem.at[s, 1]),
        )

    def kv_remote(s):
        return (
            remote(kown.at[s], koth.at[s], sent.at[0], kv_recv.at[s, 0], partner),
            remote(vown.at[s], voth.at[s], sent.at[1], kv_recv.at[s, 1], partner),
        )

    def columns(slot, dc):
        dy, dx = ORDER[slot]
        start = peer(dy, dx, dc) * COLS
        return w_hbm.at[:, pl.ds(pl.multiple_of(start, COLS), COLS)]

    def w_local(slot):
        return pltpu.make_async_copy(columns(slot, 0), wown.at[slot], wl_sem.at[0])

    def w_staged(slot):
        return pltpu.make_async_copy(columns(slot, 1), wsend.at[slot], wl_sem.at[1])

    def nkv_remote():
        return (
            remote(nk.at[half], nk.at[half], sent.at[2], nkv_recv.at[0], partner),
            remote(nv.at[half], nv.at[half], sent.at[3], nkv_recv.at[1], partner),
        )

    def wait_bytes(ref, sem):
        pltpu.make_async_copy(ref, ref, sem).wait()

    def share_remote(s, slot):
        return remote(
            psend.at[s, slot], precv.at[s, slot], sent.at[4], p_recv.at[s, slot // 4], partner
        )

    def first_remote(s):
        return (
            remote(pbuf.at[s, SLOT[2, 0], 0], r1.at[s, 0], sent.at[5], r1_recv.at[s, 0], up),
            remote(pbuf.at[s, SLOT[2, 1], 0], r1.at[s, 1], sent.at[5], r1_recv.at[s, 1], down),
        )

    def direct_remote(s):
        return (
            remote(pbuf.at[s, SLOT[1, 1], 0], r2.at[s, 1], sent.at[5], r2_recv.at[s, 1], up),
            remote(pbuf.at[s, SLOT[3, 0], 0], r2.at[s, 2], sent.at[5], r2_recv.at[s, 2], down),
        )

    def forward_remote(s):
        return (
            remote(fbuf.at[s, 0], r2.at[s, 0], sent.at[6], r2_recv.at[s, 0], up),
            remote(fbuf.at[s, 1], r2.at[s, 3], sent.at[6], r2_recv.at[s, 3], down),
        )

    def x_remote(s):
        return remote(xbuf.at[s], rx.at[s], sent.at[7], x_recv.at[s], across)

    def x_first_remote(s, dy):
        return remote(
            pbuf.at[s, SLOT[dy, 1], 1], rxx.at[s, dy], sent.at[5], xx_recv.at[s, dy], across
        )

    def y_last_remote():
        return tuple(
            remote(cbuf.at[LAST, i], q3.at[i], sent.at[8], q3_recv.at[i], dev)
            for i, dev in enumerate((far, up, down))
        )

    def tall(ref, s, i, low):
        return ref.at[s, i, pl.ds(low * TALL, TALL)]

    def y_first_remote(s):
        return (
            remote(tall(cbuf, s, 0, 0), q1.at[s, 0], sent.at[10], q1_recv.at[s, 0], up),
            remote(tall(cbuf, s, 0, 1), q1.at[s, 1], sent.at[10], q1_recv.at[s, 1], down),
        )

    def y_direct_remote(s):
        return (
            remote(tall(cbuf, s, 1, 1), tall(q2, s, 0, 1), sent.at[11], q2_recv.at[s, 1], up),
            remote(tall(cbuf, s, 2, 0), tall(q2, s, 1, 0), sent.at[11], q2_recv.at[s, 2], down),
        )

    def y_forward_remote(s):
        return (
            remote(gbuf.at[s, 0], tall(q2, s, 0, 0), sent.at[12], q2_recv.at[s, 0], up),
            remote(gbuf.at[s, 1], tall(q2, s, 1, 1), sent.at[12], q2_recv.at[s, 3], down),
        )

    others = [(dy, dx, dc) for dy in range(4) for dx in range(2) for dc in range(2)][1:]

    def square_remote(i):
        return remote(ss, ssr.at[i], sent.at[9], ss_recv, peer(*others[i]))

    load = (
        pltpu.make_async_copy(q_hbm, q_v, load_sem.at[0]),
        pltpu.make_async_copy(nk_hbm, nk.at[half], load_sem.at[1]),
        pltpu.make_async_copy(nv_hbm, nv.at[half], load_sem.at[2]),
        pltpu.make_async_copy(res_hbm, res_v, load_sem.at[3]),
    )

    barrier = pltpu.get_barrier_semaphore()
    for dev in (partner, up, down, far, across):
        pl.semaphore_signal(barrier, inc=1, device_id={"tp": dev}, device_id_type=MESH)
    first_load = kv_local(0) + load[1:3] + load[:1]
    for copy in first_load:
        copy.start()
    for copy in first_load:
        copy.wait()
    for slot in range(8):
        w_staged(slot).start()
    pl.semaphore_wait(barrier, 5)

    for pair in zip(kv_remote(0), nkv_remote()):
        for copy in pair:
            copy.start()
    for copy in kv_local(1):
        copy.start()
    for slot in range(8):
        w_local(slot).start()
    for s in range(2, SEQS):
        for copy in kv_local(s):
            copy.start()
    load[3].start()

    def rows_of(s, chunk):
        part = q_v[pl.ds(pl.multiple_of(s * SPAN, SPAN), SPAN), :]
        heads = range(chunk * HEADS, (chunk + 1) * HEADS)
        return jnp.concatenate([part[:, h * HD : (h + 1) * HD] for h in heads], axis=0)

    def chunk_rows(chunk):
        return slice(chunk * ROWS, (chunk + 1) * ROWS)

    def own_half(s):
        upcoming = dot_t(rows_of(s, 0), kown[s])
        for chunk in range(CHUNKS):
            scores = upcoming
            if chunk + 1 < CHUNKS:
                upcoming = dot_t(rows_of(s, chunk + 1), kown[s])
            rows = chunk_rows(chunk)
            peak = jnp.max(scores, axis=1, keepdims=True)
            weights = jnp.exp2((scores - peak) * SCALE).astype(BF16)
            acc_ref[rows, :] = dot(weights, with_ones(vown[s]))
            m_ref[rows, :] = jnp.broadcast_to(peak, (ROWS, HD))

    def other_half(s):
        kv_remote(s)[0].wait_recv()
        tokens = pl.ds(pl.multiple_of(s * SPAN, SPAN), SPAN)

        def scores_of(chunk):
            q = rows_of(s, chunk)
            recent = dot(q, nk[:, tokens])
            row = lax.rem(lax.broadcasted_iota(jnp.int32, recent.shape, 0), SPAN)
            col = lax.broadcasted_iota(jnp.int32, recent.shape, 1)
            return dot_t(q, koth[s]), jnp.where(row >= col, recent, -jnp.inf)

        upcoming = scores_of(0)
        for chunk in range(CHUNKS):
            scores, recent = upcoming
            if chunk + 1 < CHUNKS:
                upcoming = scores_of(chunk + 1)
            rows = chunk_rows(chunk)
            old = m_ref[rows, :1]
            peak = jnp.maximum(
                jnp.max(scores, axis=1, keepdims=True), jnp.max(recent, axis=1, keepdims=True)
            )
            peak = jnp.maximum(peak, old)
            weights = jnp.exp2((scores - peak) * SCALE).astype(BF16)
            recent_weights = jnp.exp2((recent - peak) * SCALE).astype(BF16)
            mixed = acc_ref[rows, :] * jnp.exp2((old - peak) * SCALE)
            if chunk == 0:
                kv_remote(s)[1].wait_recv()
            mixed = mixed + dot(weights, with_ones(voth[s]))
            mixed = mixed + dot_t(recent_weights, with_ones(nv[:, tokens], 0))
            result = (mixed[:, :HD] / mixed[:, HD:]).astype(BF16)
            for i in range(HEADS):
                h = chunk * HEADS + i
                aown[s, :, h * HD : (h + 1) * HD] = result[i * SPAN : (i + 1) * SPAN, :]

    def wide(ref):
        return ref.astype(F32)

    def share(s):
        for group in GROUPS:
            for slot in group:
                psend[s, slot] = dot(aown[s], wsend[slot]).astype(BF16)
            for slot in group:
                share_remote(s, slot).start()

    def project(s):
        for group in GROUPS:
            blocks = [dot(aown[s], wown[slot]) for slot in group]
            wait_bytes(precv.at[s, pl.ds(group[0], 4)], p_recv.at[s, group[0] // 4])
            for slot, block in zip(group, blocks):
                block = (block + wide(precv[s, slot])).astype(BF16)
                pbuf[s, slot, 0] = block[:, :WIDE]
                pbuf[s, slot, 1] = block[:, WIDE:]
            for slot in group:
                dy, dx = ORDER[slot]
                if dx == 1:
                    x_first_remote(s, dy).start()
                if dy == 2:
                    first_remote(s)[dx].start()
                elif (dy, dx) == (1, 1):
                    direct_remote(s)[0].start()
                elif (dy, dx) == (3, 0):
                    direct_remote(s)[1].start()

    def forward(s):
        for i, slot in enumerate((SLOT[1, 0], SLOT[3, 1])):
            first_remote(s)[i].wait_recv()
            fbuf[s, i] = (wide(r1[s, i]) + wide(pbuf[s, slot, 0])).astype(BF16)
            forward_remote(s)[i].start()

    def send_across(s):
        direct_remote(s)[0].wait_recv()
        forward_remote(s)[1].wait_recv()
        total = wide(pbuf[s, SLOT[0, 1], 0]) + wide(r2[s, 1]) + wide(r2[s, 3])
        xbuf[s] = total.astype(BF16)
        x_remote(s).start()

    def sum_across(s, last=False):
        for i, dy in enumerate((2, 1, 3)):
            x_first_remote(s, dy).wait_recv()
            cbuf[s, i] = (wide(pbuf[s, SLOT[dy, 0], 1]) + wide(rxx[s, dy])).astype(BF16)
            if last:
                y_last_remote()[i].start()
            elif i == 0:
                for copy in y_first_remote(s):
                    copy.start()
            else:
                y_direct_remote(s)[i - 1].start()

    def y_forward(s):
        for i in range(2):
            y_first_remote(s)[i].wait_recv()
            kept = wide(cbuf[s, 1 + i, i * TALL : (i + 1) * TALL, :])
            gbuf[s, i] = (wide(q1[s, i]) + kept).astype(BF16)
            y_forward_remote(s)[i].start()

    def finish(s):
        tokens = pl.ds(pl.multiple_of(s * SPAN, SPAN), SPAN)
        x_first_remote(s, 0).wait_recv()
        right = wide(pbuf[s, SLOT[0, 0], 1]) + wide(rxx[s, 0])
        if s == LAST:
            for i, copy in enumerate(y_last_remote()):
                copy.wait_recv()
                right = right + wide(q3[i])
        else:
            for copy in y_direct_remote(s) + y_forward_remote(s):
                copy.wait_recv()
            right = right + wide(q2[s, 0]) + wide(q2[s, 1])
        right = right + wide(res_v[tokens, WIDE:])
        hid[s, :, WIDE:] = right
        direct_remote(s)[1].wait_recv()
        forward_remote(s)[0].wait_recv()
        left = wide(pbuf[s, SLOT[0, 0], 0]) + wide(r2[s, 0]) + wide(r2[s, 2])
        left = left + wide(res_v[tokens, :WIDE])
        x_remote(s).wait_recv()
        left = left + wide(rx[s])
        hid[s, :, :WIDE] = left
        column = jnp.sum(left * left + right * right, axis=1, keepdims=True)
        ss[s : s + 1, :] = jnp.transpose(jnp.broadcast_to(column, (SPAN, SPAN)))[:1, :]

    own_half(0)
    for copy in kv_local(1):
        copy.wait()
    for copy in kv_remote(1):
        copy.start()
    for copy in nkv_remote():
        copy.wait_recv()

    def sequence(s, carry):
        other_half(s)

        @pl.when(s == 0)
        def _():
            wait_bytes(wown, wl_sem.at[0])
            wait_bytes(wsend, wl_sem.at[1])

        share(s)

        @pl.when(s < SEQS - 2)
        def _():
            for copy in kv_local(s + 2):
                copy.wait()
            for copy in kv_remote(s + 2):
                copy.start()

        @pl.when((s >= 1) & (s < SEQS - 1))
        def _():
            own_half(s + 1)

        @pl.when(s >= 1)
        def _():
            forward(s - 1)

        @pl.when(s >= 2)
        def _():
            send_across(s - 2)

        project(s)

        @pl.when(s == 0)
        def _():
            own_half(1)

        @pl.when(s >= 1)
        def _():
            sum_across(s - 1)

        @pl.when(s >= 2)
        def _():
            y_forward(s - 2)

        return carry

    lax.fori_loop(0, SEQS, sequence, 0)

    load[3].wait()
    ss[...] = jnp.zeros_like(ss)
    finish(0)
    forward(3)
    send_across(2)
    y_forward(2)
    finish(1)
    sum_across(LAST, last=True)
    send_across(3)
    finish(2)
    finish(3)

    for i in range(15):
        square_remote(i).start()

    sources = (
        kown, vown, nk.at[half], nv.at[half], psend, pbuf.at[:, pl.ds(0, 4)], fbuf, xbuf,
        cbuf.at[LAST], ssr, q1, q1, gbuf,
    )
    for i, ref in enumerate(sources):
        if ref is not ssr:
            wait_bytes(ref, sent.at[i])

    lines = gain_ref[...].astype(F32)
    gain = jnp.concatenate([lines[i : i + 1, :] for i in range(4)], axis=1)
    wait_bytes(ssr, ss_recv)
    squares = ss[...]
    for i in range(15):
        squares = squares + ssr[i]
    rows = lax.rsqrt(squares * (1.0 / D) + EPSILON)
    for s in range(SEQS):
        column = jnp.transpose(jnp.broadcast_to(rows[s : s + 1, :], (SPAN, SPAN)))[:, :1]
        out_ref[s * SPAN : (s + 1) * SPAN, :] = (hid[s] * column * gain).astype(BF16)
    wait_bytes(ssr, sent.at[9])


def per_device(queries, new_keys, new_values, cache_keys, cache_values, out_weight, residual, gain):
    any_spec = pl.BlockSpec(memory_space=pl.ANY)
    vmem_spec = pl.BlockSpec(memory_space=pltpu.VMEM)
    dma = pltpu.SemaphoreType.DMA
    block = (SPAN, WIDE)
    return pl.pallas_call(
        kernel,
        name="attend",
        out_shape=pltpu.VMEM((SEQS * SPAN, COLS), BF16),
        in_specs=[any_spec] * 7 + [vmem_spec],
        out_specs=vmem_spec,
        scratch_shapes=[
            pltpu.VMEM((SEQS * SPAN, 4 * HD), BF16),
            *[pltpu.VMEM((SEQS, HALF, HD), BF16)] * 4,
            *[pltpu.VMEM((HD, SEQS * SPAN), BF16)] * 2,
            *[pltpu.VMEM((8, COLS, COLS), BF16)] * 2,
            pltpu.VMEM((4 * SPAN, HD), F32),
            pltpu.VMEM((4 * SPAN, 2 * HD), F32),
            pltpu.VMEM((SEQS, SPAN, COLS), BF16),
            *[pltpu.VMEM((SEQS, 8, SPAN, COLS), BF16)] * 2,
            pltpu.VMEM((SEQS, 8, 2, *block), BF16),
            pltpu.VMEM((SEQS, 2, *block), BF16),
            pltpu.VMEM((SEQS, *block), BF16),
            pltpu.VMEM((SEQS, 2, *block), BF16),
            pltpu.VMEM((SEQS, 4, *block), BF16),
            pltpu.VMEM((SEQS, *block), BF16),
            pltpu.VMEM((SEQS, 4, *block), BF16),
            pltpu.VMEM((SEQS, 3, *block), BF16),
            *[pltpu.VMEM((LAST, 2, TALL, WIDE), BF16)] * 2,
            pltpu.VMEM((LAST, 2, *block), BF16),
            pltpu.VMEM((3, *block), BF16),
            pltpu.VMEM((SEQS, SPAN, COLS), F32),
            pltpu.VMEM((SEQS * SPAN, COLS), BF16),
            pltpu.VMEM((8, SPAN), F32),
            pltpu.VMEM((15, 8, SPAN), F32),
            dma((4,)), dma((SEQS, 2)), dma((2,)), dma((13,)), dma((SEQS, 2)), dma((2,)),
            dma((SEQS, 2)), dma((SEQS, 2)), dma((SEQS, 4)), dma((SEQS,)), dma((SEQS, 4)),
            dma((LAST, 2)), dma((LAST, 4)), dma((3,)), dma,
        ],
        compiler_params=pltpu.CompilerParams(
            collective_id=0, has_side_effects=True, vmem_limit_bytes=60 * 2**20
        ),
    )(
        queries, new_keys.T, new_values.T, cache_keys, cache_values, out_weight, residual,
        gain.reshape(4, 128),
    )


def solution(mesh):
    in_specs = (
        P("dp", "tp"),
        P("dp", "tp"),
        P("dp", "tp"),
        P("dp", "tp", None),
        P("dp", "tp", None),
        P("tp", None),
        P("dp", "tp"),
        P("tp"),
    )
    return jax.shard_map(
        per_device, mesh=mesh, in_specs=in_specs, out_specs=P("dp", "tp"), check_vma=False
    )
```

```python
import jax
import jax.numpy as jnp
from jax import lax
from jax.experimental import pallas as pl
from jax.experimental.pallas import tpu as pltpu
from jax.sharding import PartitionSpec as P

D = 8192
HD = 128
SPAN = 128
SEQS = 4
HALF = 2048
COLS = 512
EPSILON = 1e-05
SCALE = HD**-0.5 * 1.4426950408889634

MESH = pl.DeviceIdType.MESH
F32 = jnp.float32
BF16 = jnp.bfloat16

ORDER = ((2, 1), (2, 0), (1, 1), (3, 0), (3, 1), (0, 1), (1, 0), (0, 0))
SLOT = {key: slot for slot, key in enumerate(ORDER)}
WIDE = COLS // 2
TALL = SPAN // 2
LAST = SEQS - 1
GROUPS = ((0, 1, 2, 3), (4, 5, 6, 7))
HEADS = 2
ROWS = HEADS * SPAN
CHUNKS = 4 // HEADS


def dot_t(a, b):
    return lax.dot_general(a, b, (((1,), (1,)), ((), ())), preferred_element_type=F32)


def dot(a, b):
    return jnp.dot(a, b, preferred_element_type=F32)


def with_ones(v, axis=1):
    return jnp.concatenate([v, jnp.ones_like(v)], axis=axis)


def kernel(
    q_hbm, nk_hbm, nv_hbm, ck_hbm, cv_hbm, w_hbm, res_hbm, gain_ref, out_ref,
    q_v, kown, vown, koth, voth, nk, nv, wown, wsend, m_ref, acc_ref, aown, psend, precv,
    pbuf, fbuf, xbuf, r1, r2, rx, rxx, cbuf, gbuf, q1, q2, q3,
    hid, res_v, ss, ssr,
    load_sem, kvl_sem, wl_sem, sent, kv_recv, nkv_recv, p_recv,
    r1_recv, r2_recv, x_recv, xx_recv, q1_recv, q2_recv, q3_recv, ss_recv,
):
    me = lax.axis_index("tp")
    core = lax.rem(me, 2)
    xh = lax.rem(lax.div(me, 2), 2)
    y = lax.div(me, 4)
    half = pl.ds(pl.multiple_of(core * (HD // 2), HD // 2), HD // 2)

    def peer(dy, dx, dc):
        py = lax.rem(y + dy, 4)
        px = lax.rem(xh + dx, 2)
        pc = lax.rem(core + dc, 2)
        return (py * 2 + px) * 2 + pc

    partner = peer(0, 0, 1)
    up, down, far, across = peer(1, 0, 0), peer(3, 0, 0), peer(2, 0, 0), peer(0, 1, 0)

    def remote(src, dst, send, recv, dev):
        return pltpu.make_async_remote_copy(
            src_ref=src, dst_ref=dst, send_sem=send, recv_sem=recv,
            device_id={"tp": dev}, device_id_type=MESH,
        )

    def kv_local(s):
        return (
            pltpu.make_async_copy(ck_hbm.at[s], kown.at[s], kvl_sem.at[s, 0]),
            pltpu.make_async_copy(cv_hbm.at[s], vown.at[s], kvl_sem.at[s, 1]),
        )

    def kv_remote(s):
        return (
            remote(kown.at[s], koth.at[s], sent.at[0], kv_recv.at[s, 0], partner),
            remote(vown.at[s], voth.at[s], sent.at[1], kv_recv.at[s, 1], partner),
        )

    def columns(slot, dc):
        dy, dx = ORDER[slot]
        start = peer(dy, dx, dc) * COLS
        return w_hbm.at[:, pl.ds(pl.multiple_of(start, COLS), COLS)]

    def w_local(slot):
        return pltpu.make_async_copy(columns(slot, 0), wown.at[slot], wl_sem.at[0])

    def w_staged(slot):
        return pltpu.make_async_copy(columns(slot, 1), wsend.at[slot], wl_sem.at[1])

    def nkv_remote():
        return (
            remote(nk.at[half], nk.at[half], sent.at[2], nkv_recv.at[0], partner),
            remote(nv.at[half], nv.at[half], sent.at[3], nkv_recv.at[1], partner),
        )

    def wait_bytes(ref, sem):
        pltpu.make_async_copy(ref, ref, sem).wait()

    def share_remote(s, slot):
        return remote(
            psend.at[s, slot], precv.at[s, slot], sent.at[4], p_recv.at[s, slot // 4], partner
        )

    def first_remote(s):
        return (
            remote(pbuf.at[s, SLOT[2, 0], 0], r1.at[s, 0], sent.at[5], r1_recv.at[s, 0], up),
            remote(pbuf.at[s, SLOT[2, 1], 0], r1.at[s, 1], sent.at[5], r1_recv.at[s, 1], down),
        )

    def direct_remote(s):
        return (
            remote(pbuf.at[s, SLOT[1, 1], 0], r2.at[s, 1], sent.at[5], r2_recv.at[s, 1], up),
            remote(pbuf.at[s, SLOT[3, 0], 0], r2.at[s, 2], sent.at[5], r2_recv.at[s, 2], down),
        )

    def forward_remote(s):
        return (
            remote(fbuf.at[s, 0], r2.at[s, 0], sent.at[6], r2_recv.at[s, 0], up),
            remote(fbuf.at[s, 1], r2.at[s, 3], sent.at[6], r2_recv.at[s, 3], down),
        )

    def x_remote(s):
        return remote(xbuf.at[s], rx.at[s], sent.at[7], x_recv.at[s], across)

    def x_first_remote(s, dy):
        return remote(
            pbuf.at[s, SLOT[dy, 1], 1], rxx.at[s, dy], sent.at[5], xx_recv.at[s, dy], across
        )

    def y_last_remote():
        return tuple(
            remote(cbuf.at[LAST, i], q3.at[i], sent.at[8], q3_recv.at[i], dev)
            for i, dev in enumerate((far, up, down))
        )

    def tall(ref, s, i, low):
        return ref.at[s, i, pl.ds(low * TALL, TALL)]

    def y_first_remote(s):
        return (
            remote(tall(cbuf, s, 0, 0), q1.at[s, 0], sent.at[10], q1_recv.at[s, 0], up),
            remote(tall(cbuf, s, 0, 1), q1.at[s, 1], sent.at[10], q1_recv.at[s, 1], down),
        )

    def y_direct_remote(s):
        return (
            remote(tall(cbuf, s, 1, 1), tall(q2, s, 0, 1), sent.at[11], q2_recv.at[s, 1], up),
            remote(tall(cbuf, s, 2, 0), tall(q2, s, 1, 0), sent.at[11], q2_recv.at[s, 2], down),
        )

    def y_forward_remote(s):
        return (
            remote(gbuf.at[s, 0], tall(q2, s, 0, 0), sent.at[12], q2_recv.at[s, 0], up),
            remote(gbuf.at[s, 1], tall(q2, s, 1, 1), sent.at[12], q2_recv.at[s, 3], down),
        )

    others = [(dy, dx, dc) for dy in range(4) for dx in range(2) for dc in range(2)][1:]

    def square_remote(i):
        return remote(ss, ssr.at[i], sent.at[9], ss_recv, peer(*others[i]))

    load = (
        pltpu.make_async_copy(q_hbm, q_v, load_sem.at[0]),
        pltpu.make_async_copy(nk_hbm, nk.at[half], load_sem.at[1]),
        pltpu.make_async_copy(nv_hbm, nv.at[half], load_sem.at[2]),
        pltpu.make_async_copy(res_hbm, res_v, load_sem.at[3]),
    )

    barrier = pltpu.get_barrier_semaphore()
    for dev in (partner, up, down, far, across):
        pl.semaphore_signal(barrier, inc=1, device_id={"tp": dev}, device_id_type=MESH)
    first_load = kv_local(0) + load[1:3] + load[:1]
    for copy in first_load:
        copy.start()
    for copy in first_load:
        copy.wait()
    for slot in range(8):
        w_staged(slot).start()
    pl.semaphore_wait(barrier, 5)

    for pair in zip(kv_remote(0), nkv_remote()):
        for copy in pair:
            copy.start()
    for copy in kv_local(1):
        copy.start()
    for slot in range(8):
        w_local(slot).start()
    for s in range(2, SEQS):
        for copy in kv_local(s):
            copy.start()
    load[3].start()

    def rows_of(s, chunk):
        part = q_v[pl.ds(pl.multiple_of(s * SPAN, SPAN), SPAN), :]
        heads = range(chunk * HEADS, (chunk + 1) * HEADS)
        return jnp.concatenate([part[:, h * HD : (h + 1) * HD] for h in heads], axis=0)

    def chunk_rows(chunk):
        return slice(chunk * ROWS, (chunk + 1) * ROWS)

    def own_half(s):
        upcoming = dot_t(rows_of(s, 0), kown[s])
        for chunk in range(CHUNKS):
            scores = upcoming
            if chunk + 1 < CHUNKS:
                upcoming = dot_t(rows_of(s, chunk + 1), kown[s])
            rows = chunk_rows(chunk)
            peak = jnp.max(scores, axis=1, keepdims=True)
            weights = jnp.exp2((scores - peak) * SCALE).astype(BF16)
            acc_ref[rows, :] = dot(weights, with_ones(vown[s]))
            m_ref[rows, :] = jnp.broadcast_to(peak, (ROWS, HD))

    def other_half(s):
        kv_remote(s)[0].wait_recv()
        tokens = pl.ds(pl.multiple_of(s * SPAN, SPAN), SPAN)

        def scores_of(chunk):
            q = rows_of(s, chunk)
            recent = dot(q, nk[:, tokens])
            row = lax.rem(lax.broadcasted_iota(jnp.int32, recent.shape, 0), SPAN)
            col = lax.broadcasted_iota(jnp.int32, recent.shape, 1)
            return dot_t(q, koth[s]), jnp.where(row >= col, recent, -jnp.inf)

        upcoming = scores_of(0)
        for chunk in range(CHUNKS):
            scores, recent = upcoming
            if chunk + 1 < CHUNKS:
                upcoming = scores_of(chunk + 1)
            rows = chunk_rows(chunk)
            old = m_ref[rows, :1]
            peak = jnp.maximum(
                jnp.max(scores, axis=1, keepdims=True), jnp.max(recent, axis=1, keepdims=True)
            )
            peak = jnp.maximum(peak, old)
            weights = jnp.exp2((scores - peak) * SCALE).astype(BF16)
            recent_weights = jnp.exp2((recent - peak) * SCALE).astype(BF16)
            mixed = acc_ref[rows, :] * jnp.exp2((old - peak) * SCALE)
            if chunk == 0:
                kv_remote(s)[1].wait_recv()
            mixed = mixed + dot(weights, with_ones(voth[s]))
            mixed = mixed + dot_t(recent_weights, with_ones(nv[:, tokens], 0))
            result = (mixed[:, :HD] / mixed[:, HD:]).astype(BF16)
            for i in range(HEADS):
                h = chunk * HEADS + i
                aown[s, :, h * HD : (h + 1) * HD] = result[i * SPAN : (i + 1) * SPAN, :]

    def wide(ref):
        return ref.astype(F32)

    def share(s):
        for group in GROUPS:
            for slot in group:
                psend[s, slot] = dot(aown[s], wsend[slot]).astype(BF16)
            for slot in group:
                share_remote(s, slot).start()

    def project(s):
        for group in GROUPS:
            blocks = [dot(aown[s], wown[slot]) for slot in group]
            wait_bytes(precv.at[s, pl.ds(group[0], 4)], p_recv.at[s, group[0] // 4])
            for slot, block in zip(group, blocks):
                block = (block + wide(precv[s, slot])).astype(BF16)
                pbuf[s, slot, 0] = block[:, :WIDE]
                pbuf[s, slot, 1] = block[:, WIDE:]
            for slot in group:
                dy, dx = ORDER[slot]
                if dx == 1:
                    x_first_remote(s, dy).start()
                if dy == 2:
                    first_remote(s)[dx].start()
                elif (dy, dx) == (1, 1):
                    direct_remote(s)[0].start()
                elif (dy, dx) == (3, 0):
                    direct_remote(s)[1].start()

    def forward(s):
        for i, slot in enumerate((SLOT[1, 0], SLOT[3, 1])):
            first_remote(s)[i].wait_recv()
            fbuf[s, i] = (wide(r1[s, i]) + wide(pbuf[s, slot, 0])).astype(BF16)
            forward_remote(s)[i].start()

    def send_across(s):
        direct_remote(s)[0].wait_recv()
        forward_remote(s)[1].wait_recv()
        total = wide(pbuf[s, SLOT[0, 1], 0]) + wide(r2[s, 1]) + wide(r2[s, 3])
        xbuf[s] = total.astype(BF16)
        x_remote(s).start()

    def sum_across(s, last=False):
        for i, dy in enumerate((2, 1, 3)):
            x_first_remote(s, dy).wait_recv()
            cbuf[s, i] = (wide(pbuf[s, SLOT[dy, 0], 1]) + wide(rxx[s, dy])).astype(BF16)
            if last:
                y_last_remote()[i].start()
            elif i == 0:
                for copy in y_first_remote(s):
                    copy.start()
            else:
                y_direct_remote(s)[i - 1].start()

    def y_forward(s):
        for i in range(2):
            y_first_remote(s)[i].wait_recv()
            kept = wide(cbuf[s, 1 + i, i * TALL : (i + 1) * TALL, :])
            gbuf[s, i] = (wide(q1[s, i]) + kept).astype(BF16)
            y_forward_remote(s)[i].start()

    def finish(s):
        tokens = pl.ds(pl.multiple_of(s * SPAN, SPAN), SPAN)
        x_first_remote(s, 0).wait_recv()
        right = wide(pbuf[s, SLOT[0, 0], 1]) + wide(rxx[s, 0])
        if s == LAST:
            for i, copy in enumerate(y_last_remote()):
                copy.wait_recv()
                right = right + wide(q3[i])
        else:
            for copy in y_direct_remote(s) + y_forward_remote(s):
                copy.wait_recv()
            right = right + wide(q2[s, 0]) + wide(q2[s, 1])
        right = right + wide(res_v[tokens, WIDE:])
        hid[s, :, WIDE:] = right
        direct_remote(s)[1].wait_recv()
        forward_remote(s)[0].wait_recv()
        left = wide(pbuf[s, SLOT[0, 0], 0]) + wide(r2[s, 0]) + wide(r2[s, 2])
        left = left + wide(res_v[tokens, :WIDE])
        x_remote(s).wait_recv()
        left = left + wide(rx[s])
        hid[s, :, :WIDE] = left
        column = jnp.sum(left * left + right * right, axis=1, keepdims=True)
        ss[s : s + 1, :] = jnp.transpose(jnp.broadcast_to(column, (SPAN, SPAN)))[:1, :]

    own_half(0)
    for copy in kv_local(1):
        copy.wait()
    for copy in kv_remote(1):
        copy.start()
    for copy in nkv_remote():
        copy.wait_recv()

    def sequence(s, carry):
        other_half(s)

        @pl.when(s == 0)
        def _():
            wait_bytes(wown, wl_sem.at[0])
            wait_bytes(wsend, wl_sem.at[1])

        share(s)

        @pl.when(s < SEQS - 2)
        def _():
            for copy in kv_local(s + 2):
                copy.wait()
            for copy in kv_remote(s + 2):
                copy.start()

        @pl.when((s >= 1) & (s < SEQS - 1))
        def _():
            own_half(s + 1)

        @pl.when(s >= 1)
        def _():
            forward(s - 1)

        @pl.when(s >= 2)
        def _():
            send_across(s - 2)

        project(s)

        @pl.when(s == 0)
        def _():
            own_half(1)

        @pl.when(s >= 2)
        def _():
            y_forward(s - 2)

        @pl.when(s >= 1)
        def _():
            sum_across(s - 1)

        return carry

    lax.fori_loop(0, SEQS, sequence, 0)

    load[3].wait()
    ss[...] = jnp.zeros_like(ss)
    finish(0)
    forward(3)
    send_across(2)
    y_forward(2)
    finish(1)
    sum_across(LAST, last=True)
    send_across(3)
    finish(2)
    finish(3)

    for i in range(15):
        square_remote(i).start()

    sources = (
        kown, vown, nk.at[half], nv.at[half], psend, pbuf.at[:, pl.ds(0, 4)], fbuf, xbuf,
        cbuf.at[LAST], ssr, q1, q1, gbuf,
    )
    for i, ref in enumerate(sources):
        if ref is not ssr:
            wait_bytes(ref, sent.at[i])

    lines = gain_ref[...].astype(F32)
    gain = jnp.concatenate([lines[i : i + 1, :] for i in range(4)], axis=1)
    wait_bytes(ssr, ss_recv)
    squares = ss[...]
    for i in range(15):
        squares = squares + ssr[i]
    rows = lax.rsqrt(squares * (1.0 / D) + EPSILON)
    for s in range(SEQS):
        column = jnp.transpose(jnp.broadcast_to(rows[s : s + 1, :], (SPAN, SPAN)))[:, :1]
        out_ref[s * SPAN : (s + 1) * SPAN, :] = (hid[s] * column * gain).astype(BF16)
    wait_bytes(ssr, sent.at[9])


def per_device(queries, new_keys, new_values, cache_keys, cache_values, out_weight, residual, gain):
    any_spec = pl.BlockSpec(memory_space=pl.ANY)
    vmem_spec = pl.BlockSpec(memory_space=pltpu.VMEM)
    dma = pltpu.SemaphoreType.DMA
    block = (SPAN, WIDE)
    return pl.pallas_call(
        kernel,
        name="attend",
        out_shape=pltpu.VMEM((SEQS * SPAN, COLS), BF16),
        in_specs=[any_spec] * 7 + [vmem_spec],
        out_specs=vmem_spec,
        scratch_shapes=[
            pltpu.VMEM((SEQS * SPAN, 4 * HD), BF16),
            *[pltpu.VMEM((SEQS, HALF, HD), BF16)] * 4,
            *[pltpu.VMEM((HD, SEQS * SPAN), BF16)] * 2,
            *[pltpu.VMEM((8, COLS, COLS), BF16)] * 2,
            pltpu.VMEM((4 * SPAN, HD), F32),
            pltpu.VMEM((4 * SPAN, 2 * HD), F32),
            pltpu.VMEM((SEQS, SPAN, COLS), BF16),
            *[pltpu.VMEM((SEQS, 8, SPAN, COLS), BF16)] * 2,
            pltpu.VMEM((SEQS, 8, 2, *block), BF16),
            pltpu.VMEM((SEQS, 2, *block), BF16),
            pltpu.VMEM((SEQS, *block), BF16),
            pltpu.VMEM((SEQS, 2, *block), BF16),
            pltpu.VMEM((SEQS, 4, *block), BF16),
            pltpu.VMEM((SEQS, *block), BF16),
            pltpu.VMEM((SEQS, 4, *block), BF16),
            pltpu.VMEM((SEQS, 3, *block), BF16),
            *[pltpu.VMEM((LAST, 2, TALL, WIDE), BF16)] * 2,
            pltpu.VMEM((LAST, 2, *block), BF16),
            pltpu.VMEM((3, *block), BF16),
            pltpu.VMEM((SEQS, SPAN, COLS), F32),
            pltpu.VMEM((SEQS * SPAN, COLS), BF16),
            pltpu.VMEM((8, SPAN), F32),
            pltpu.VMEM((15, 8, SPAN), F32),
            dma((4,)), dma((SEQS, 2)), dma((2,)), dma((13,)), dma((SEQS, 2)), dma((2,)),
            dma((SEQS, 2)), dma((SEQS, 2)), dma((SEQS, 4)), dma((SEQS,)), dma((SEQS, 4)),
            dma((LAST, 2)), dma((LAST, 4)), dma((3,)), dma,
        ],
        compiler_params=pltpu.CompilerParams(
            collective_id=0, has_side_effects=True, vmem_limit_bytes=60 * 2**20
        ),
    )(
        queries, new_keys.T, new_values.T, cache_keys, cache_values, out_weight, residual,
        gain.reshape(4, 128),
    )


def solution(mesh):
    in_specs = (
        P("dp", "tp"),
        P("dp", "tp"),
        P("dp", "tp"),
        P("dp", "tp", None),
        P("dp", "tp", None),
        P("tp", None),
        P("dp", "tp"),
        P("tp"),
    )
    return jax.shard_map(
        per_device, mesh=mesh, in_specs=in_specs, out_specs=P("dp", "tp"), check_vma=False
    )
```

```python
import jax
import jax.numpy as jnp
from jax import lax
from jax.experimental import pallas as pl
from jax.experimental.pallas import tpu as pltpu
from jax.sharding import PartitionSpec as P

D = 8192
HD = 128
SPAN = 128
SEQS = 4
HALF = 2048
COLS = 512
EPSILON = 1e-05
SCALE = HD**-0.5 * 1.4426950408889634

MESH = pl.DeviceIdType.MESH
F32 = jnp.float32
BF16 = jnp.bfloat16

ORDER = ((2, 1), (2, 0), (1, 1), (3, 0), (3, 1), (0, 1), (1, 0), (0, 0))
SLOT = {key: slot for slot, key in enumerate(ORDER)}
WIDE = COLS // 2
TALL = SPAN // 2
LAST = SEQS - 1
GROUPS = ((0, 1, 2, 3), (4, 5, 6, 7))
HEADS = 2
ROWS = HEADS * SPAN
CHUNKS = 4 // HEADS


def dot_t(a, b):
    return lax.dot_general(a, b, (((1,), (1,)), ((), ())), preferred_element_type=F32)


def dot(a, b):
    return jnp.dot(a, b, preferred_element_type=F32)


def with_ones(v, axis=1):
    return jnp.concatenate([v, jnp.ones_like(v)], axis=axis)


def kernel(
    q_hbm, nk_hbm, nv_hbm, ck_hbm, cv_hbm, w_hbm, res_hbm, gain_ref, out_ref,
    q_v, kown, vown, koth, voth, nk, nv, wown, wsend, m_ref, acc_ref, aown, psend, precv,
    pbuf, fbuf, xbuf, r1, r2, rx, rxx, cbuf, gbuf, q1, q2, q3,
    hid, res_v, ss, ssr,
    load_sem, kvl_sem, wl_sem, sent, kv_recv, nkv_recv, p_recv,
    r1_recv, r2_recv, x_recv, xx_recv, q1_recv, q2_recv, q3_recv, ss_recv,
):
    me = lax.axis_index("tp")
    core = lax.rem(me, 2)
    xh = lax.rem(lax.div(me, 2), 2)
    y = lax.div(me, 4)
    half = pl.ds(pl.multiple_of(core * (HD // 2), HD // 2), HD // 2)

    def peer(dy, dx, dc):
        py = lax.rem(y + dy, 4)
        px = lax.rem(xh + dx, 2)
        pc = lax.rem(core + dc, 2)
        return (py * 2 + px) * 2 + pc

    partner = peer(0, 0, 1)
    up, down, far, across = peer(1, 0, 0), peer(3, 0, 0), peer(2, 0, 0), peer(0, 1, 0)

    def remote(src, dst, send, recv, dev):
        return pltpu.make_async_remote_copy(
            src_ref=src, dst_ref=dst, send_sem=send, recv_sem=recv,
            device_id={"tp": dev}, device_id_type=MESH,
        )

    def kv_local(s):
        return (
            pltpu.make_async_copy(ck_hbm.at[s], kown.at[s], kvl_sem.at[s, 0]),
            pltpu.make_async_copy(cv_hbm.at[s], vown.at[s], kvl_sem.at[s, 1]),
        )

    def kv_remote(s):
        return (
            remote(kown.at[s], koth.at[s], sent.at[0], kv_recv.at[s, 0], partner),
            remote(vown.at[s], voth.at[s], sent.at[1], kv_recv.at[s, 1], partner),
        )

    def columns(slot, dc):
        dy, dx = ORDER[slot]
        start = peer(dy, dx, dc) * COLS
        return w_hbm.at[:, pl.ds(pl.multiple_of(start, COLS), COLS)]

    def w_local(slot):
        return pltpu.make_async_copy(columns(slot, 0), wown.at[slot], wl_sem.at[0])

    def w_staged(slot):
        return pltpu.make_async_copy(columns(slot, 1), wsend.at[slot], wl_sem.at[1])

    def nkv_remote():
        return (
            remote(nk.at[half], nk.at[half], sent.at[2], nkv_recv.at[0], partner),
            remote(nv.at[half], nv.at[half], sent.at[3], nkv_recv.at[1], partner),
        )

    def wait_bytes(ref, sem):
        pltpu.make_async_copy(ref, ref, sem).wait()

    def share_remote(s, slot):
        return remote(
            psend.at[s, slot], precv.at[s, slot], sent.at[4], p_recv.at[s, slot // 4], partner
        )

    def first_remote(s):
        return (
            remote(pbuf.at[s, SLOT[2, 0], 0], r1.at[s, 0], sent.at[5], r1_recv.at[s, 0], up),
            remote(pbuf.at[s, SLOT[2, 1], 0], r1.at[s, 1], sent.at[5], r1_recv.at[s, 1], down),
        )

    def direct_remote(s):
        return (
            remote(pbuf.at[s, SLOT[1, 1], 0], r2.at[s, 1], sent.at[5], r2_recv.at[s, 1], up),
            remote(pbuf.at[s, SLOT[3, 0], 0], r2.at[s, 2], sent.at[5], r2_recv.at[s, 2], down),
        )

    def forward_remote(s):
        return (
            remote(fbuf.at[s, 0], r2.at[s, 0], sent.at[6], r2_recv.at[s, 0], up),
            remote(fbuf.at[s, 1], r2.at[s, 3], sent.at[6], r2_recv.at[s, 3], down),
        )

    def x_remote(s):
        return remote(xbuf.at[s], rx.at[s], sent.at[7], x_recv.at[s], across)

    def x_first_remote(s, dy):
        return remote(
            pbuf.at[s, SLOT[dy, 1], 1], rxx.at[s, dy], sent.at[5], xx_recv.at[s, dy], across
        )

    def y_last_remote():
        return tuple(
            remote(cbuf.at[LAST, i], q3.at[i], sent.at[8], q3_recv.at[i], dev)
            for i, dev in enumerate((far, up, down))
        )

    def tall(ref, s, i, low):
        return ref.at[s, i, pl.ds(low * TALL, TALL)]

    def y_first_remote(s):
        return (
            remote(tall(cbuf, s, 0, 0), q1.at[s, 0], sent.at[10], q1_recv.at[s, 0], up),
            remote(tall(cbuf, s, 0, 1), q1.at[s, 1], sent.at[10], q1_recv.at[s, 1], down),
        )

    def y_direct_remote(s):
        return (
            remote(tall(cbuf, s, 1, 1), tall(q2, s, 0, 1), sent.at[11], q2_recv.at[s, 1], up),
            remote(tall(cbuf, s, 2, 0), tall(q2, s, 1, 0), sent.at[11], q2_recv.at[s, 2], down),
        )

    def y_forward_remote(s):
        return (
            remote(gbuf.at[s, 0], tall(q2, s, 0, 0), sent.at[12], q2_recv.at[s, 0], up),
            remote(gbuf.at[s, 1], tall(q2, s, 1, 1), sent.at[12], q2_recv.at[s, 3], down),
        )

    others = [(dy, dx, dc) for dy in range(4) for dx in range(2) for dc in range(2)][:0:-1]

    def square_remote(i):
        return remote(ss, ssr.at[i], sent.at[9], ss_recv, peer(*others[i]))

    load = (
        pltpu.make_async_copy(q_hbm, q_v, load_sem.at[0]),
        pltpu.make_async_copy(nk_hbm, nk.at[half], load_sem.at[1]),
        pltpu.make_async_copy(nv_hbm, nv.at[half], load_sem.at[2]),
        pltpu.make_async_copy(res_hbm, res_v, load_sem.at[3]),
    )

    barrier = pltpu.get_barrier_semaphore()
    for dev in (partner, up, down, far, across):
        pl.semaphore_signal(barrier, inc=1, device_id={"tp": dev}, device_id_type=MESH)
    first_load = kv_local(0) + load[1:3] + load[:1]
    for copy in first_load:
        copy.start()
    for copy in first_load:
        copy.wait()
    for slot in range(8):
        w_staged(slot).start()
    pl.semaphore_wait(barrier, 5)

    for copy in kv_remote(0)[:1] + nkv_remote() + kv_remote(0)[1:]:
        copy.start()
    for copy in kv_local(1):
        copy.start()
    for slot in range(8):
        w_local(slot).start()
    for s in range(2, SEQS):
        for copy in kv_local(s):
            copy.start()
    load[3].start()

    def rows_of(s, chunk):
        part = q_v[pl.ds(pl.multiple_of(s * SPAN, SPAN), SPAN), :]
        heads = range(chunk * HEADS, (chunk + 1) * HEADS)
        return jnp.concatenate([part[:, h * HD : (h + 1) * HD] for h in heads], axis=0)

    def chunk_rows(chunk):
        return slice(chunk * ROWS, (chunk + 1) * ROWS)

    def own_half(s):
        upcoming = dot_t(rows_of(s, 0), kown[s])
        for chunk in range(CHUNKS):
            scores = upcoming
            if chunk + 1 < CHUNKS:
                upcoming = dot_t(rows_of(s, chunk + 1), kown[s])
            rows = chunk_rows(chunk)
            peak = jnp.max(scores, axis=1, keepdims=True)
            weights = jnp.exp2((scores - peak) * SCALE).astype(BF16)
            acc_ref[rows, :] = dot(weights, with_ones(vown[s]))
            m_ref[rows, :] = jnp.broadcast_to(peak, (ROWS, HD))

    def other_half(s):
        kv_remote(s)[0].wait_recv()
        tokens = pl.ds(pl.multiple_of(s * SPAN, SPAN), SPAN)

        def scores_of(chunk):
            q = rows_of(s, chunk)
            recent = dot(q, nk[:, tokens])
            row = lax.rem(lax.broadcasted_iota(jnp.int32, recent.shape, 0), SPAN)
            col = lax.broadcasted_iota(jnp.int32, recent.shape, 1)
            return dot_t(q, koth[s]), jnp.where(row >= col, recent, -jnp.inf)

        upcoming = scores_of(0)
        for chunk in range(CHUNKS):
            scores, recent = upcoming
            if chunk + 1 < CHUNKS:
                upcoming = scores_of(chunk + 1)
            rows = chunk_rows(chunk)
            old = m_ref[rows, :1]
            peak = jnp.maximum(
                jnp.max(scores, axis=1, keepdims=True), jnp.max(recent, axis=1, keepdims=True)
            )
            peak = jnp.maximum(peak, old)
            weights = jnp.exp2((scores - peak) * SCALE).astype(BF16)
            recent_weights = jnp.exp2((recent - peak) * SCALE).astype(BF16)
            mixed = acc_ref[rows, :] * jnp.exp2((old - peak) * SCALE)
            if chunk == 0:
                kv_remote(s)[1].wait_recv()
            mixed = mixed + dot(weights, with_ones(voth[s]))
            mixed = mixed + dot_t(recent_weights, with_ones(nv[:, tokens], 0))
            result = (mixed[:, :HD] / mixed[:, HD:]).astype(BF16)
            for i in range(HEADS):
                h = chunk * HEADS + i
                aown[s, :, h * HD : (h + 1) * HD] = result[i * SPAN : (i + 1) * SPAN, :]

    def wide(ref):
        return ref.astype(F32)

    def share(s):
        for group in GROUPS:
            for slot in group:
                psend[s, slot] = dot(aown[s], wsend[slot]).astype(BF16)
            for slot in group:
                share_remote(s, slot).start()

    def project(s):
        for group in GROUPS:
            blocks = [dot(aown[s], wown[slot]) for slot in group]
            wait_bytes(precv.at[s, pl.ds(group[0], 4)], p_recv.at[s, group[0] // 4])
            for slot, block in zip(group, blocks):
                block = (block + wide(precv[s, slot])).astype(BF16)
                pbuf[s, slot, 0] = block[:, :WIDE]
                pbuf[s, slot, 1] = block[:, WIDE:]
            for slot in group:
                dy, dx = ORDER[slot]
                if dx == 1:
                    x_first_remote(s, dy).start()
                if dy == 2:
                    first_remote(s)[dx].start()
                elif (dy, dx) == (1, 1):
                    direct_remote(s)[0].start()
                elif (dy, dx) == (3, 0):
                    direct_remote(s)[1].start()

    def forward(s):
        for i, slot in enumerate((SLOT[1, 0], SLOT[3, 1])):
            first_remote(s)[i].wait_recv()
            fbuf[s, i] = (wide(r1[s, i]) + wide(pbuf[s, slot, 0])).astype(BF16)
            forward_remote(s)[i].start()

    def send_across(s):
        direct_remote(s)[0].wait_recv()
        forward_remote(s)[1].wait_recv()
        total = wide(pbuf[s, SLOT[0, 1], 0]) + wide(r2[s, 1]) + wide(r2[s, 3])
        xbuf[s] = total.astype(BF16)
        x_remote(s).start()

    def sum_across(s, last=False):
        for i, dy in enumerate((2, 1, 3)):
            x_first_remote(s, dy).wait_recv()
            cbuf[s, i] = (wide(pbuf[s, SLOT[dy, 0], 1]) + wide(rxx[s, dy])).astype(BF16)
            if last:
                y_last_remote()[i].start()
            elif i == 0:
                for copy in y_first_remote(s):
                    copy.start()
            else:
                y_direct_remote(s)[i - 1].start()

    def y_forward(s):
        for i in range(2):
            y_first_remote(s)[i].wait_recv()
            kept = wide(cbuf[s, 1 + i, i * TALL : (i + 1) * TALL, :])
            gbuf[s, i] = (wide(q1[s, i]) + kept).astype(BF16)
            y_forward_remote(s)[i].start()

    def finish(s):
        tokens = pl.ds(pl.multiple_of(s * SPAN, SPAN), SPAN)
        x_first_remote(s, 0).wait_recv()
        right = wide(pbuf[s, SLOT[0, 0], 1]) + wide(rxx[s, 0])
        if s == LAST:
            for i, copy in enumerate(y_last_remote()):
                copy.wait_recv()
                right = right + wide(q3[i])
        else:
            for copy in y_direct_remote(s) + y_forward_remote(s):
                copy.wait_recv()
            right = right + wide(q2[s, 0]) + wide(q2[s, 1])
        right = right + wide(res_v[tokens, WIDE:])
        hid[s, :, WIDE:] = right
        direct_remote(s)[1].wait_recv()
        forward_remote(s)[0].wait_recv()
        left = wide(pbuf[s, SLOT[0, 0], 0]) + wide(r2[s, 0]) + wide(r2[s, 2])
        left = left + wide(res_v[tokens, :WIDE])
        x_remote(s).wait_recv()
        left = left + wide(rx[s])
        hid[s, :, :WIDE] = left
        column = jnp.sum(left * left + right * right, axis=1, keepdims=True)
        ss[s : s + 1, :] = jnp.transpose(jnp.broadcast_to(column, (SPAN, SPAN)))[:1, :]

    own_half(0)
    for copy in kv_local(1):
        copy.wait()
    for copy in kv_remote(1):
        copy.start()
    for copy in nkv_remote():
        copy.wait_recv()

    def sequence(s, carry):
        other_half(s)

        @pl.when(s == 0)
        def _():
            wait_bytes(wown, wl_sem.at[0])
            wait_bytes(wsend, wl_sem.at[1])

        share(s)

        @pl.when(s < SEQS - 2)
        def _():
            for copy in kv_local(s + 2):
                copy.wait()
            for copy in kv_remote(s + 2):
                copy.start()

        @pl.when((s >= 1) & (s < SEQS - 1))
        def _():
            own_half(s + 1)

        @pl.when(s >= 1)
        def _():
            forward(s - 1)

        @pl.when(s >= 2)
        def _():
            send_across(s - 2)

        project(s)

        @pl.when(s == 0)
        def _():
            own_half(1)

        @pl.when(s >= 1)
        def _():
            sum_across(s - 1)

        @pl.when(s >= 2)
        def _():
            y_forward(s - 2)

        return carry

    lax.fori_loop(0, SEQS, sequence, 0)

    load[3].wait()
    ss[...] = jnp.zeros_like(ss)
    finish(0)
    forward(3)
    send_across(2)
    y_forward(2)
    finish(1)
    sum_across(LAST, last=True)
    send_across(3)
    finish(2)
    finish(3)

    for i in range(15):
        square_remote(i).start()

    sources = (
        kown, vown, nk.at[half], nv.at[half], psend, pbuf.at[:, pl.ds(0, 4)], fbuf, xbuf,
        cbuf.at[LAST], ssr, q1, q1, gbuf,
    )
    for i, ref in enumerate(sources):
        if ref is not ssr:
            wait_bytes(ref, sent.at[i])

    lines = gain_ref[...].astype(F32)
    gain = jnp.concatenate([lines[i : i + 1, :] for i in range(4)], axis=1)
    wait_bytes(ssr, ss_recv)
    squares = ss[...]
    for i in range(15):
        squares = squares + ssr[i]
    rows = lax.rsqrt(squares * (1.0 / D) + EPSILON)
    for s in range(SEQS):
        column = jnp.transpose(jnp.broadcast_to(rows[s : s + 1, :], (SPAN, SPAN)))[:, :1]
        out_ref[s * SPAN : (s + 1) * SPAN, :] = (hid[s] * column * gain).astype(BF16)
    wait_bytes(ssr, sent.at[9])


def per_device(queries, new_keys, new_values, cache_keys, cache_values, out_weight, residual, gain):
    any_spec = pl.BlockSpec(memory_space=pl.ANY)
    vmem_spec = pl.BlockSpec(memory_space=pltpu.VMEM)
    dma = pltpu.SemaphoreType.DMA
    block = (SPAN, WIDE)
    return pl.pallas_call(
        kernel,
        name="attend",
        out_shape=pltpu.VMEM((SEQS * SPAN, COLS), BF16),
        in_specs=[any_spec] * 7 + [vmem_spec],
        out_specs=vmem_spec,
        scratch_shapes=[
            pltpu.VMEM((SEQS * SPAN, 4 * HD), BF16),
            *[pltpu.VMEM((SEQS, HALF, HD), BF16)] * 4,
            *[pltpu.VMEM((HD, SEQS * SPAN), BF16)] * 2,
            *[pltpu.VMEM((8, COLS, COLS), BF16)] * 2,
            pltpu.VMEM((4 * SPAN, HD), F32),
            pltpu.VMEM((4 * SPAN, 2 * HD), F32),
            pltpu.VMEM((SEQS, SPAN, COLS), BF16),
            *[pltpu.VMEM((SEQS, 8, SPAN, COLS), BF16)] * 2,
            pltpu.VMEM((SEQS, 8, 2, *block), BF16),
            pltpu.VMEM((SEQS, 2, *block), BF16),
            pltpu.VMEM((SEQS, *block), BF16),
            pltpu.VMEM((SEQS, 2, *block), BF16),
            pltpu.VMEM((SEQS, 4, *block), BF16),
            pltpu.VMEM((SEQS, *block), BF16),
            pltpu.VMEM((SEQS, 4, *block), BF16),
            pltpu.VMEM((SEQS, 3, *block), BF16),
            *[pltpu.VMEM((LAST, 2, TALL, WIDE), BF16)] * 2,
            pltpu.VMEM((LAST, 2, *block), BF16),
            pltpu.VMEM((3, *block), BF16),
            pltpu.VMEM((SEQS, SPAN, COLS), F32),
            pltpu.VMEM((SEQS * SPAN, COLS), BF16),
            pltpu.VMEM((8, SPAN), F32),
            pltpu.VMEM((15, 8, SPAN), F32),
            dma((4,)), dma((SEQS, 2)), dma((2,)), dma((13,)), dma((SEQS, 2)), dma((2,)),
            dma((SEQS, 2)), dma((SEQS, 2)), dma((SEQS, 4)), dma((SEQS,)), dma((SEQS, 4)),
            dma((LAST, 2)), dma((LAST, 4)), dma((3,)), dma,
        ],
        compiler_params=pltpu.CompilerParams(
            collective_id=0, has_side_effects=True, vmem_limit_bytes=60 * 2**20
        ),
    )(
        queries, new_keys.T, new_values.T, cache_keys, cache_values, out_weight, residual,
        gain.reshape(4, 128),
    )


def solution(mesh):
    in_specs = (
        P("dp", "tp"),
        P("dp", "tp"),
        P("dp", "tp"),
        P("dp", "tp", None),
        P("dp", "tp", None),
        P("tp", None),
        P("dp", "tp"),
        P("tp"),
    )
    return jax.shard_map(
        per_device, mesh=mesh, in_specs=in_specs, out_specs=P("dp", "tp"), check_vma=False
    )
```
